128 devices in a mesh: gx: 4 (over x), gy: 32 (over y, z, core).
Axes of the slice: x: 4, y: 4, z: 4, core: 2. Of those that a mesh axis runs over, the one named last changes fastest.
Arguments:
- replay_deter: float32 [32768, 2048], P(('gx', 'gy')), may hold values from -1 to 1
- replay_stoch: int32 [32768, 32], P(('gx', 'gy')), may hold values from 0 to 31
- send_rows: int32 [16384, 2], P(('gx', 'gy')), may hold values from 0 to 255
- send_counts: int32 [128, 128], P(('gx', 'gy')), may hold values from 0 to 2, as said below
- actions: int32 [32768, 4], P(('gx', 'gy')), may hold values from 0 to 17
- samples: int32 [32768, 4, 32], P(('gx', 'gy')), may hold values from 0 to 31
- w_stoch: bfloat16 [1024, 6144], P('gy'), may hold values from -1 to 1
- w_deter: bfloat16 [4, 512, 1536], P(None, 'gy'), may hold values from -0.25 to 0.25
- act_table: bfloat16 [18, 6144], replicated, may hold values from -3 to 3
- w_prior: bfloat16 [2048, 1024], P('gy'), may hold values from -0.037353516 to 0.037353516
Outputs:
- imagined: bfloat16 [32768, 4, 2048], P(('gx', 'gy'))
- log_prob: float32 [32768, 4, 32], P(('gx', 'gy'))
The draws below stay inside these ranges and needn't reach their ends.
Inputs may be any that keep to these rules, and one draw needn't show every extreme that they name: `send_rows`: entries past a destination's count are unused. `send_counts`: each source's counts sum to exactly 128; every source sends 2 rows to some owner, and some owner receives 2 rows from every source.
All inputs are finite; a program needn't handle non-finite values.
Results may differ from the reference program's by a relative error of at most 0.0022.
Values may be sent and summed in bfloat16 or wider, within the bound.
A program may use at most 128 MiB of HBM per device.

```python
import jax
import jax.numpy as jnp
from jax import lax

GROUPS = 32
CLASSES = 32
BLOCKS = 4
BLOCK_W = 512
DETER = 2048
ACTIONS = 18
STEPS = 4
LENGTH = 64
SEQ_DEV = 4
SLOTS = 256
CAP = 2
LIVE = 128
DEVICES = 128


def draw_send_counts(key, part):
    frequent_choices = jax.random.randint(jax.random.fold_in(key, 11), (DEVICES,), 0, 6144)
    gumbel_jitter = jax.random.randint(jax.random.fold_in(key, 12), (DEVICES, DEVICES, CAP), 0, 4096)
    preference_boost = jax.random.randint(jax.random.fold_in(key, 13), (DEVICES,), 0, DEVICES)
    overfull_slots = jax.random.randint(jax.random.fold_in(key, 14), (), 0, DEVICES)
    owning_devices = jnp.arange(DEVICES, dtype=jnp.int32)
    extra_reward = jnp.where(owning_devices[None, :] == preference_boost[:, None], 16384, 0) + jnp.where(owning_devices[None, :] == overfull_slots, 12288, 0)
    ranking_score = gumbel_jitter + frequent_choices[None, :, None] + extra_reward[:, :, None]
    width = DEVICES * CAP
    keyed = ranking_score.reshape(DEVICES, width) * width + jnp.arange(width, dtype=jnp.int32)[None, :]
    best, chosen = lax.top_k(keyed, LIVE)
    picked = jnp.zeros((DEVICES, width), jnp.int32).at[jnp.arange(DEVICES)[:, None], chosen].set(1)
    return picked.reshape(DEVICES, DEVICES, CAP).sum(-1).astype(jnp.int32)


def with_ends(drawn, stream_key, low, high):
    index_at = [jax.random.randint(jax.random.fold_in(stream_key, axis), (), 0, length) for axis, length in enumerate(drawn.shape)]
    main_axis = drawn.shape.index(max(drawn.shape))
    next_to = index_at[:main_axis] + [(index_at[main_axis] + 1) % drawn.shape[main_axis]] + index_at[main_axis + 1:]
    return drawn.at[tuple(index_at)].set(low).at[tuple(next_to)].set(high)


def shard_levels(own_key, dims, pieces, least, high):
    level, own = 1.0, jax.random.fold_in(own_key, 6)
    for dim, parts in pieces:
        heights = jnp.exp(jax.random.uniform(jax.random.fold_in(own, dim), (parts,), jnp.float32, least / len(pieces), high / len(pieces)))
        level = level * jnp.repeat(heights, dims[dim] // parts).reshape([-1 if axis == dim else 1 for axis in range(len(dims))])
    return level


def centred(own_key, shape, deviation, limit, pieces=(), kind=jnp.bfloat16):
    gain = shard_levels(own_key, shape, pieces, -0.22, 0.18) if pieces else 1.0
    array = jax.random.normal(own_key, shape, jnp.float32) * deviation * gain
    return jnp.minimum(jnp.maximum(array, -limit), limit).astype(kind)


def setup_inputs(seed: int = 0) -> dict:
    keys = jax.random.split(jax.random.key(seed), 11)
    return {
        "replay_deter": jnp.clip(jax.random.uniform(keys[0], (DEVICES * SEQ_DEV * LENGTH, DETER), jnp.float32, -1.0, 1.0) * shard_levels(keys[0], (DEVICES * SEQ_DEV * LENGTH, DETER), ((0, 128),), -0.4, 0.0), -1.0, 1.0),
        "replay_stoch": with_ends(jax.random.randint(keys[1], (DEVICES * SEQ_DEV * LENGTH, GROUPS), 0, CLASSES), jax.random.fold_in(keys[1], 1), 0, CLASSES - 1).astype(jnp.int32),
        "send_rows": with_ends(jax.random.randint(keys[2], (DEVICES * DEVICES, CAP), 0, SEQ_DEV * LENGTH), jax.random.fold_in(keys[2], 1), 0, (SEQ_DEV * LENGTH) - 1).astype(jnp.int32),
        "send_counts": draw_send_counts(jax.random.fold_in(keys[10], 71), 0),
        "actions": with_ends(jax.random.randint(keys[4], (DEVICES * SLOTS, STEPS), 0, ACTIONS), jax.random.fold_in(keys[4], 1), 0, ACTIONS - 1).astype(jnp.int32),
        "samples": with_ends(jax.random.randint(keys[5], (DEVICES * SLOTS, STEPS, GROUPS), 0, CLASSES), jax.random.fold_in(keys[5], 1), 0, CLASSES - 1).astype(jnp.int32),
        "w_stoch": centred(keys[6], (GROUPS * CLASSES, 3 * DETER), GROUPS ** -0.5, 1.0, ((0, 32),)),
        "w_deter": centred(keys[7], (BLOCKS, BLOCK_W, 3 * BLOCK_W), BLOCK_W ** -0.5, 0.25, ((1, 32),)),
        "act_table": centred(keys[8], (ACTIONS, 3 * DETER), 0.5, 3.0),
        "w_prior": jnp.clip(jax.random.uniform(keys[9], (DETER, GROUPS * CLASSES), jnp.float32, -0.037353516, 0.037353516) * shard_levels(keys[9], (DETER, GROUPS * CLASSES), ((0, 32),), -0.4, 0.0), -0.037353516, 0.037353516).astype(jnp.bfloat16),
    }


def gru_step(state, stoch, action, w_stoch, w_deter, act_table):
    rows = state.shape[0]
    state_low = state.astype(jnp.bfloat16)
    onehot = (stoch[:, :, None] == jnp.arange(CLASSES, dtype=jnp.int32)[None, None, :]).reshape(rows, GROUPS * CLASSES).astype(jnp.bfloat16)
    act_hot = (action[:, None] == jnp.arange(ACTIONS, dtype=jnp.int32)[None, :]).astype(jnp.bfloat16)
    gates = jnp.dot(onehot, w_stoch, preferred_element_type=jnp.float32) + jnp.dot(act_hot, act_table, preferred_element_type=jnp.float32)
    gates = gates.reshape(rows, BLOCKS, 3 * BLOCK_W)
    blocked = state_low.reshape(rows, BLOCKS, BLOCK_W).astype(jnp.float32)
    gates = gates + jnp.einsum("rbi,bio->rbo", blocked, w_deter.astype(jnp.float32))
    reset = jax.nn.sigmoid(gates[..., :BLOCK_W])
    cand = jnp.tanh(reset * gates[..., BLOCK_W:2 * BLOCK_W])
    update = jax.nn.sigmoid(gates[..., 2 * BLOCK_W:] - 1.0)
    before = state.reshape(rows, BLOCKS, BLOCK_W)
    return (update * cand + (1.0 - update) * before).reshape(rows, BLOCKS * BLOCK_W)


def imagine(start, first, acts, samps, w_stoch, w_deter, act_table):
    state = start
    stoch = first
    states = []
    for step in range(STEPS):
        state = gru_step(state, stoch, acts[:, step], w_stoch, w_deter, act_table)
        states.append(state.astype(jnp.bfloat16))
        stoch = samps[:, step]
    return jnp.stack(states, 1)


def prior_logp(states, samps, w_prior):
    rows = states.shape[0]
    logits = jnp.dot(states.reshape(rows * STEPS, DETER), w_prior, preferred_element_type=jnp.float32)
    logits = logits.reshape(rows, STEPS, GROUPS, CLASSES)
    totals = jnp.log(jnp.sum(jnp.exp(logits), -1))
    hits = samps[..., None] == jnp.arange(CLASSES, dtype=jnp.int32)
    picked = jnp.sum(jnp.where(hits, logits, jnp.zeros_like(logits)), -1)
    return picked - totals


def reference(replay_deter, replay_stoch, send_rows, send_counts, actions, samples, w_stoch, w_deter, act_table, w_prior):
    count = DEVICES
    rows_dev = SEQ_DEV * LENGTH
    lists = send_rows.reshape(count, count, CAP)
    offsets = (jnp.arange(count, dtype=jnp.int32) * rows_dev)[:, None, None]
    global_rows = jnp.transpose(lists + offsets, (1, 0, 2)).astype(jnp.int32)
    live = jnp.arange(CAP, dtype=jnp.int32)[None, None, :] < jnp.transpose(send_counts)[:, :, None]
    acts_all = actions.reshape(count, SLOTS, STEPS)
    samps_all = samples.reshape(count, SLOTS, STEPS, GROUPS)

    def one_owner(inputs):
        picks, mask, acts, samps = inputs
        picks = picks.reshape(SLOTS)
        mask = mask.reshape(SLOTS)
        start = replay_deter[picks]
        first = replay_stoch[picks]
        states = imagine(start, first, acts, samps, w_stoch, w_deter, act_table)
        states = jnp.where(mask[:, None, None], states, jnp.zeros_like(states))
        logp = prior_logp(states, samps, w_prior)
        logp = jnp.where(mask[:, None, None], logp, jnp.zeros_like(logp))
        return states, logp

    states, logp = lax.map(one_owner, (global_rows, live, acts_all, samps_all))
    return states.reshape(count * SLOTS, STEPS, DETER), logp.reshape(count * SLOTS, STEPS, GROUPS)
```

```python
import jax
import jax.numpy as jnp
from jax import lax
from jax.experimental import pallas as pl
from jax.experimental.pallas import tpu as pltpu
from jax.sharding import PartitionSpec as P

STEPS = 4
BLOCKS = 4
BF = jnp.bfloat16
F32 = jnp.float32
MESH = pl.DeviceIdType.MESH
SCALE = 32767.0


def dot(a, b, dims=((1,), (0,))):
    return lax.dot_general(a, b, (dims, ((), ())), preferred_element_type=F32)


def spread(rows, lanes):
    g = lax.broadcasted_iota(jnp.int32, (rows, lanes), 0)
    k = lax.broadcasted_iota(jnp.int32, (rows, lanes), 1)
    return jnp.where((k >= g * 32) & (k < g * 32 + 32), 1.0, 0.0).astype(BF)


def sig(v):
    return 0.5 * jnp.tanh(0.5 * v) + 0.5


def gru_kernel(
    deter, stoch_t, rows_t, counts, acts_t, samps_t, w_s, w_d, act, w_p,
    st_out, wp_out, live_out,
    WS, WD, WP, send, recv, send_z, recv_z, zf, H0, H, OH, ACT, PRE, ST,
    s_loc, s_snd, s_rcv, g_snd, g_rcv, f_snd, f_rcv, wp_snd, wp_rcv, d_snd, d_rcv, s_out,
):
    x = lax.axis_index("gx")
    gy = lax.axis_index("gy")
    y, z, c = gy // 8, (gy // 2) % 4, gy % 2
    me = x * 32 + gy

    def dev(tx, ty, tz, tc):
        return (tx, ty * 8 + tz * 2 + tc)

    def near(dim, step):
        s = (step + 4) % 4
        if dim == "x":
            return dev((x + s) % 4, y, z, c)
        if dim == "y":
            return dev(x, (y + s) % 4, z, c)
        return dev(x, y, (z + s) % 4, c)

    pos = {"x": x, "y": y, "z": z}
    partner = dev(x, y, z, 1 - c)

    def fill(b, wait):
        def go(src, dst, k):
            cp = pltpu.make_async_copy(src, dst, s_loc.at[k])
            if not wait:
                cp.start()

        for p in range(3):
            for q in range(4) if p == 0 else (x,):
                col = pl.multiple_of(b * 1536 + p * 512 + q * 128, 128)
                go(w_s.at[:, pl.ds(col, 128)], WS.at[b, p, q, y, z, c], 0)
                col2 = pl.multiple_of(p * 512 + q * 128, 128)
                go(w_d.at[b, :, pl.ds(col2, 128)], WD.at[b, p, q, y, z, c], 1)
        return 0

    lax.fori_loop(0, 4, lambda b, u: fill(b, False), 0)
    for j in range(8):
        if j < 3:
            for q in range(4):
                pltpu.make_async_copy(
                    w_p.at[pl.ds(q * 16, 16), pl.ds(j * 128, 128)], WP.at[j, y, z, c, q], s_loc.at[2]
                ).start()
        else:
            pltpu.make_async_copy(
                w_p.at[pl.ds(pl.multiple_of(x * 16, 16), 16), pl.ds(j * 128, 128)],
                WP.at[j, y, z, c, x],
                s_loc.at[3],
            ).start()

    iota = lax.broadcasted_iota(jnp.int32, (256, 128), 0)
    sel_t = jnp.concatenate(
        [jnp.where(iota == rows_t[i : i + 1, :], 1.0, 0.0) for i in range(2)], axis=1
    )
    sel = jnp.transpose(sel_t).astype(BF)
    for k in range(8):
        lo = 512 * (k // 2) + 128 * (k % 2)
        parts = []
        for col in (lo, lo + 256):
            code = jnp.round(deter[:, col : col + 128] * SCALE)
            high = jnp.floor(code * (1.0 / 256.0))
            parts += [high.astype(BF), (code - high * 256.0).astype(BF)]
        got = dot(sel, jnp.concatenate(parts, axis=1))
        v0 = (got[:, 0:128] * 256.0 + got[:, 128:256]).astype(jnp.int32)
        v1 = (got[:, 256:384] * 256.0 + got[:, 384:512]).astype(jnp.int32)
        word = v1 * 65536 + (v0 + 32768)
        send[pl.ds(k, 128, stride=16), :] = word[0:128]
        send[pl.ds(8 + k, 128, stride=16), :] = word[128:256]
    picked = dot(stoch_t[...].astype(F32).astype(BF), sel_t.astype(BF))
    zs = [
        jnp.where(counts[...] > i, picked[:, 128 * i : 128 * i + 128], 64.0) for i in range(2)
    ]
    zs = jnp.concatenate(zs + [jnp.zeros((64, 128), F32)], axis=0)
    send_z[...] = jnp.transpose(zs).astype(jnp.int32).reshape(128, 1, 128)

    def wait_bytes(ref, sem):
        pltpu.make_async_copy(ref, ref, sem).wait()

    wait_bytes(WS.at[0, :, :, 0:2, 0, 0], s_loc.at[0])
    wait_bytes(WD.at[0, :, :, 0:2, 0, 0], s_loc.at[1])
    wait_bytes(WP.at[0:3, 0, 0, 0], s_loc.at[2])
    wait_bytes(WP.at[0:5, 0, 0, 0, 0], s_loc.at[3])

    def copy_to(ref, snd, rcv, to):
        return pltpu.make_async_remote_copy(
            src_ref=ref, dst_ref=ref, send_sem=snd, recv_sem=rcv, device_id=to, device_id_type=MESH
        )

    class Ring:
        def __init__(self, dim, part, half, snd, rcv):
            self.dim, self.part, self.half, self.snd, self.rcv = dim, part, half, snd, rcv

        def at(self, step):
            return (pos[self.dim] + step + 4) % 4

        def copy(self, k):
            if k < 2:
                ref = self.part(self.at(0))
            else:
                ref = self.half(self.at(-1 if k == 2 else 1), k - 2)
            return copy_to(ref, self.snd.at[k], self.rcv.at[k], near(self.dim, 1 if k % 2 == 0 else -1))

        def came(self, k):
            if k < 2:
                ref = self.part(self.at(-1 if k == 0 else 1))
            else:
                ref = self.half(self.at(2), k - 2)
            return copy_to(ref, self.snd.at[k], self.rcv.at[k], near(self.dim, 1 if k % 2 == 0 else -1))

        def start(self):
            self.copy(0).start()
            self.copy(1).start()

        def mid(self):
            for k in range(2):
                self.came(k).wait_recv()
                self.copy(2 + k).start()

        def end(self):
            for k in range(2):
                self.came(2 + k).wait_recv()

        def sent(self):
            for k in range(4):
                self.copy(k).wait_send()

    def early(i, dim, parts):
        return [Ring(dim, part, half, g_snd.at[i, a], g_rcv.at[i, a]) for a, (part, half) in enumerate(parts)]

    hs = (slice(0, 2), slice(2, 4))
    a_y = early(0, "y", [
        (lambda i: WS.at[:, 0, :, i, z, c], lambda i, h: WS.at[hs[h], 0, :, i, z, c]),
        (lambda i: WD.at[:, 0, :, i, z, c], lambda i, h: WD.at[hs[h], 0, :, i, z, c]),
        (lambda i: WP.at[0:3, i, z, c], lambda i, h: WP.at[0:3, i, z, c, hs[h]]),
    ])
    b_y = early(1, "y", [
        (lambda i: WS.at[:, 1, x, i, z, c], lambda i, h: WS.at[hs[h], 1, x, i, z, c]),
        (lambda i: WD.at[:, 1, x, i, z, c], lambda i, h: WD.at[hs[h], 1, x, i, z, c]),
        (lambda i: WP.at[3:6, i, z, c, x], lambda i, h: WP.at[slice(3, 4) if h == 0 else slice(4, 6), i, z, c, x]),
    ])
    c_z = early(2, "z", [
        (lambda i: WS.at[:, 2, x, y, i, c], lambda i, h: WS.at[hs[h], 2, x, y, i, c]),
        (lambda i: WD.at[:, 2, x, y, i, c], lambda i, h: WD.at[hs[h], 2, x, y, i, c]),
        (lambda i: WP.at[6:8, y, i, c, x], lambda i, h: WP.at[6 + h : 7 + h, y, i, c, x]),
    ])
    b_z = early(3, "z", [
        (lambda i: WS.at[:, 1, x, :, i, c], lambda i, h: WS.at[hs[h], 1, x, :, i, c]),
        (lambda i: WD.at[:, 1, x, :, i, c], lambda i, h: WD.at[hs[h], 1, x, :, i, c]),
        (lambda i: WP.at[3:6, :, i, c, x], lambda i, h: WP.at[3:6, hs[h], i, c, x]),
    ])
    c_x = early(4, "x", [
        (lambda i: WS.at[:, 2, i, y, :, c], lambda i, h: WS.at[hs[h], 2, i, y, :, c]),
        (lambda i: WD.at[:, 2, i, y, :, c], lambda i, h: WD.at[hs[h], 2, i, y, :, c]),
        (lambda i: WP.at[6:8, y, :, c, i], lambda i, h: WP.at[6:8, y, hs[h], c, i]),
    ])

    def last(W, b, s):
        sn, rc = f_snd.at[b], f_rcv.at[b]
        return [
            Ring("z", lambda i: W.at[b, 0, :, :, i, c], lambda i, h: W.at[b, 0, hs[h], :, i, c], sn.at[0, s], rc.at[0, s]),
            Ring("x", lambda i: W.at[b, 1, i, :, :, c], lambda i, h: W.at[b, 1, i, hs[h], :, c], sn.at[1, s], rc.at[1, s]),
            Ring("y", lambda i: W.at[b, 2, :, i, :, c], lambda i, h: W.at[b, 2, hs[h], i, :, c], sn.at[2, s], rc.at[2, s]),
        ]

    def last_p():
        return [
            Ring("z", lambda i: WP.at[0:3, :, i, c], lambda i, h: WP.at[0:3, hs[h], i, c], wp_snd.at[0], wp_rcv.at[0]),
            Ring("x", lambda i: WP.at[3:6, :, :, c, i], lambda i, h: WP.at[3:6, hs[h], :, c, i], wp_snd.at[1], wp_rcv.at[1]),
            Ring("y", lambda i: WP.at[6:8, i, :, c], lambda i, h: WP.at[6:8, i, hs[h], c], wp_snd.at[2], wp_rcv.at[2]),
        ]

    class Block:
        def __init__(self, rings, whole):
            self.rings = rings
            self.whole = whole

        def over(self, ref, k):
            copy_to(ref, d_snd.at[k], d_rcv.at[k], partner).start()

        def start(self):
            for r, k in self.rings:
                r.start()
                self.over(r.part(r.at(0)), k)

        def mid(self):
            for r, k in self.rings:
                for e in range(2):
                    r.came(e).wait_recv()
                    r.copy(2 + e).start()
                    self.over(r.part(r.at(-1 if e == 0 else 1)), k)

        def end(self):
            for r, k in self.rings:
                for e in range(2):
                    r.came(2 + e).wait_recv()
                    self.over(r.half(r.at(2), e), k)

        def ready(self):
            for ref, k in self.whole:
                wait_bytes(ref(1 - c), d_rcv.at[k])

        def sent(self):
            for r, _ in self.rings:
                r.sent()
            for ref, k in self.whole:
                wait_bytes(ref(c), d_snd.at[k])

    def block(b):
        return Block(
            [(r, 2 * b) for r in last(WS, b, 0)] + [(r, 2 * b + 1) for r in last(WD, b, 1)],
            [(lambda e: WS.at[b, :, :, :, :, e], 2 * b), (lambda e: WD.at[b, :, :, :, :, e], 2 * b + 1)],
        )

    def block_p():
        return Block([(r, 8) for r in last_p()], [(lambda e: WP.at[:, :, :, e], 8)])

    for r in b_y + c_z + a_y:
        r.start()

    def rows_of(n):
        return pl.ds(pl.multiple_of(n * 16, 16), 16)

    def a2a(i):
        r = i % 32
        tx, ty, tz, tc = (x + i // 32) % 4, (y + r // 8) % 4, (z + (r // 2) % 4) % 4, (c + r % 2) % 2
        to = dev(tx, ty, tz, tc)
        n = tx * 32 + ty * 8 + tz * 2 + tc
        return (
            pltpu.make_async_remote_copy(
                src_ref=send.at[rows_of(n), :], dst_ref=recv.at[rows_of(me), :],
                send_sem=s_snd.at[0], recv_sem=s_rcv.at[0], device_id=to, device_id_type=MESH,
            ),
            pltpu.make_async_remote_copy(
                src_ref=send_z.at[n], dst_ref=recv_z.at[me],
                send_sem=s_snd.at[1], recv_sem=s_rcv.at[1], device_id=to, device_id_type=MESH,
            ),
        )

    def a2a_start(i, u):
        for cp in a2a(i):
            cp.start()
        return u

    lax.fori_loop(1, 128, a2a_start, 0)
    own = [
        pltpu.make_async_copy(send.at[rows_of(me), :], recv.at[rows_of(me), :], s_loc.at[4]),
        pltpu.make_async_copy(send_z.at[me], recv_z.at[me], s_loc.at[5]),
    ]
    for cp in own:
        cp.start()

    for r in b_y + c_z:
        r.mid()
    for r in b_y + c_z:
        r.end()
    for r in b_z + c_x:
        r.start()
    for r in a_y:
        r.mid()
    for r in a_y:
        r.end()

    E = spread(32, 1024)
    cls = (lax.broadcasted_iota(jnp.int32, (256, 1024), 1) % 32).astype(F32)
    for t in range(1, 4):
        rep = dot(samps_t[t - 1].astype(F32).astype(BF), E, ((0,), (0,)))
        OH[t] = jnp.where(rep == cls, 1.0, 0.0).astype(BF)
    ACT[...] = jnp.zeros_like(ACT)
    ACT[0 : act.shape[0], :] = act[...]

    for r in b_z + c_x:
        r.mid()
    for r in b_z + c_x:
        r.end()
    block(0).start()
    block(1).start()

    wait_bytes(recv.at[pl.ds(0, 127 * 16), :], s_rcv.at[0])
    wait_bytes(recv_z.at[pl.ds(0, 127)], s_rcv.at[1])
    for cp in own:
        cp.wait()
    zv = recv_z[...].reshape(128, 128)
    zf[pl.ds(0, 128, stride=2), :] = zv
    zf[pl.ds(1, 128, stride=2), :] = pltpu.roll(zv, 96, 1)
    codes = zf[...].astype(F32)
    rep = dot(codes[:, 0:32].astype(BF), E)
    OH[0] = jnp.where(rep == cls, 1.0, 0.0).astype(BF)
    alive = jnp.where(codes < 32.0, 1.0, 0.0)
    lane0 = jnp.where(lax.broadcasted_iota(jnp.int32, (8, 128), 1) == 0, 1.0, 0.0).astype(BF)
    live_out[...] = dot(lane0, alive.astype(BF), ((1,), (1,)))
    live_col = alive[:, 0:1]
    for k in range(8):
        word = recv[pl.ds(k, 256, stride=8), :]
        v1 = lax.shift_right_arithmetic(word, 16)
        v0 = (word & 65535) - 32768
        b, e = k // 2, (k % 2) * 128
        H0[b, :, e : e + 128] = v0.astype(F32) * (1.0 / SCALE)
        H0[b, :, 256 + e : 384 + e] = v1.astype(F32) * (1.0 / SCALE)

    block(0).mid()
    block(0).end()
    block(0).ready()

    def compute(b, u):
        def gate(p):
            def pre(t, u):
                rhs = jnp.concatenate([WS[b, p, q].reshape(1024, 128) for q in range(4)], axis=1)
                a_hot = jnp.where(
                    lax.broadcasted_iota(jnp.int32, (32, 256), 0) == acts_t[pl.ds(t, 1), :], 1.0, 0.0
                ).astype(BF)
                cols = pl.ds(pl.multiple_of(b * 1536 + p * 512, 512), 512)
                PRE[t, p] = dot(OH[t], rhs) + dot(a_hot, ACT[:, cols], ((0,), (0,)))
                return u

            lax.fori_loop(0, STEPS, pre, 0)

        gate(0)

        @pl.when(b < 2)
        def _():
            block(b + 2).start()

        @pl.when(b == 2)
        def _():
            block_p().start()

        gate(1)

        @pl.when(b < 3)
        def _():
            block(b + 1).mid()

        @pl.when(b == 3)
        def _():
            block_p().mid()

        gate(2)
        H[...] = H0[b]

        def step(t, u):
            h = H[...]
            low = h.astype(BF)

            def gates(p):
                rhs = jnp.concatenate([WD[b, p, q].reshape(512, 128) for q in range(4)], axis=1)
                return PRE[t, p] + dot(low, rhs)

            cand = jnp.tanh(sig(gates(0)) * gates(1))
            g = sig(gates(2) - 1.0)
            new = g * cand + (1.0 - g) * h
            H[...] = new
            ST[b, t] = (new * live_col).astype(BF)
            return u

        lax.fori_loop(0, STEPS, step, 0)
        pltpu.make_async_copy(ST.at[b], st_out.at[b], s_out.at[b]).start()

        @pl.when(b < 3)
        def _():
            block(b + 1).end()
            block(b + 1).ready()

        return u

    lax.fori_loop(0, BLOCKS, compute, 0)
    bp = block_p()
    bp.end()
    bp.ready()
    out_p = pltpu.make_async_copy(WP, wp_out, s_out.at[4])
    out_p.start()
    for r in a_y + b_y + c_z + b_z + c_x:
        r.sent()
    wait_bytes(send.at[pl.ds(0, 127 * 16), :], s_snd.at[0])
    wait_bytes(send_z.at[pl.ds(0, 127)], s_snd.at[1])

    def drain(b, u):
        block(b).sent()
        pltpu.make_async_copy(ST.at[b], st_out.at[b], s_out.at[b]).wait()
        return u

    lax.fori_loop(0, BLOCKS, drain, 0)
    bp.sent()
    out_p.wait()


def prior_kernel(st, wp, live, samps_t, out):
    E = spread(32, 1024)
    cls = (lax.broadcasted_iota(jnp.int32, (256, 1024), 1) % 32).astype(F32)

    def step(t, u):
        logits = jnp.zeros((256, 1024), F32)
        for b in range(BLOCKS):
            rhs = jnp.concatenate([wp[j, b].reshape(512, 128) for j in range(8)], axis=1)
            logits = logits + dot(st[b, t], rhs)
        rep = dot(samps_t[t].astype(F32).astype(BF), E, ((0,), (0,)))

        def grouped(v):
            hi = v.astype(BF)
            lo = (v - hi.astype(F32)).astype(BF)
            return dot(E, hi, ((1,), (1,))) + dot(E, lo, ((1,), (1,)))

        total = jnp.log(grouped(jnp.exp(logits)))
        hit = grouped(jnp.where(rep == cls, logits, 0.0))
        out[t] = jnp.where(live[0:1, :] > 0.0, hit - total, 0.0)
        return u

    lax.fori_loop(0, STEPS, step, 0)


def on_device(deter, stoch, rows, counts, acts, samps, w_s, w_d, act, w_p):
    vmem = pl.BlockSpec(memory_space=pltpu.VMEM)
    hbm = pl.BlockSpec(memory_space=pl.ANY)
    dma = pltpu.SemaphoreType.DMA
    samps_t = samps.transpose(1, 2, 0)
    states, wp, live = pl.pallas_call(
        gru_kernel,
        name="gru",
        out_shape=(
            jax.ShapeDtypeStruct((4, 4, 256, 512), BF),
            jax.ShapeDtypeStruct((8, 4, 4, 2, 4, 16, 128), BF),
            jax.ShapeDtypeStruct((8, 256), F32),
        ),
        in_specs=[vmem] * 6 + [hbm, hbm, vmem, hbm],
        out_specs=(hbm, hbm, vmem),
        scratch_shapes=[
            pltpu.VMEM((4, 3, 4, 4, 4, 2, 32, 128), BF),
            pltpu.VMEM((4, 3, 4, 4, 4, 2, 16, 128), BF),
            pltpu.VMEM((8, 4, 4, 2, 4, 16, 128), BF),
            pltpu.VMEM((2048, 128), jnp.int32),
            pltpu.VMEM((2048, 128), jnp.int32),
            pltpu.VMEM((128, 1, 128), jnp.int32),
            pltpu.VMEM((128, 1, 128), jnp.int32),
            pltpu.VMEM((256, 128), jnp.int32),
            pltpu.VMEM((4, 256, 512), F32),
            pltpu.VMEM((256, 512), F32),
            pltpu.VMEM((4, 256, 1024), BF),
            pltpu.VMEM((32, 6144), BF),
            pltpu.VMEM((4, 3, 256, 512), F32),
            pltpu.VMEM((4, 4, 256, 512), BF),
            dma((6,)), dma((2,)), dma((2,)),
            dma((5, 3, 4)), dma((5, 3, 4)),
            dma((4, 3, 2, 4)), dma((4, 3, 2, 4)),
            dma((3, 4)), dma((3, 4)),
            dma((9,)), dma((9,)), dma((5,)),
        ],
        compiler_params=pltpu.CompilerParams(
            has_side_effects=True, vmem_limit_bytes=60 * 1024 * 1024
        ),
    )(deter, stoch.T, rows.T, counts, acts.T, samps_t, w_s, w_d, act, w_p)
    imagined = states.transpose(2, 1, 0, 3).reshape(256, 4, 2048)
    logp = pl.pallas_call(
        prior_kernel,
        name="prior",
        out_shape=jax.ShapeDtypeStruct((4, 32, 256), F32),
        in_specs=[vmem] * 4,
        out_specs=vmem,
        compiler_params=pltpu.CompilerParams(vmem_limit_bytes=48 * 1024 * 1024),
    )(states, wp, live, samps_t)
    return (imagined, logp.transpose(2, 0, 1))


def solution(mesh):
    in_specs = (
        P(("gx", "gy"), None),
        P(("gx", "gy"), None),
        P(("gx", "gy"), None),
        P(("gx", "gy"), None),
        P(("gx", "gy"), None),
        P(("gx", "gy"), None, None),
        P("gy", None),
        P(None, "gy", None),
        P(),
        P("gy", None),
    )
    out_specs = (P(("gx", "gy"), None, None), P(("gx", "gy"), None, None))
    return jax.shard_map(
        on_device, mesh=mesh, in_specs=in_specs, out_specs=out_specs, check_vma=False
    )
```

```python
import jax
import jax.numpy as jnp
from jax import lax
from jax.experimental import pallas as pl
from jax.experimental.pallas import tpu as pltpu
from jax.sharding import PartitionSpec as P

STEPS = 4
BLOCKS = 4
BF = jnp.bfloat16
F32 = jnp.float32
MESH = pl.DeviceIdType.MESH
SCALE = 32767.0


def dot(a, b, dims=((1,), (0,))):
    return lax.dot_general(a, b, (dims, ((), ())), preferred_element_type=F32)


def spread(rows, lanes):
    g = lax.broadcasted_iota(jnp.int32, (rows, lanes), 0)
    k = lax.broadcasted_iota(jnp.int32, (rows, lanes), 1)
    return jnp.where((k >= g * 32) & (k < g * 32 + 32), 1.0, 0.0).astype(BF)


def sig(v):
    return 0.5 * jnp.tanh(0.5 * v) + 0.5


def gru_kernel(
    deter_h, stoch_t, rows_t, counts, acts_t, samps_t, w_s, w_d, act, w_p,
    st_out, wp_out, live_out,
    deter, WS, WD, WP, send, recv, send_z, recv_z, zf, H0, H, OH, ACT, PRE, ST,
    s_loc, s_snd, s_rcv, w_snd, w_rcv, p_snd, p_rcv, d_snd, d_rcv, s_out,
):
    x = lax.axis_index("gx")
    gy = lax.axis_index("gy")
    y, z, c = gy // 8, (gy // 2) % 4, gy % 2
    me = x * 32 + gy

    def dev(tx, ty, tz, tc):
        return (tx, ty * 8 + tz * 2 + tc)

    def near(dim, step):
        s = (step + 4) % 4
        if dim == "x":
            return dev((x + s) % 4, y, z, c)
        if dim == "y":
            return dev(x, (y + s) % 4, z, c)
        return dev(x, y, (z + s) % 4, c)

    pos = {"x": x, "y": y, "z": z}
    partner = dev(x, y, z, 1 - c)

    def wait_bytes(ref, sem):
        pltpu.make_async_copy(ref, ref, sem).wait()

    get_deter = pltpu.make_async_copy(deter_h, deter, s_loc.at[6])

    def fill(b, u):
        for p in range(3):
            for q in range(4) if p == 0 else (x,):
                col = pl.multiple_of(b * 1536 + p * 512 + q * 128, 128)
                pltpu.make_async_copy(
                    w_s.at[:, pl.ds(col, 128)], WS.at[b, p, q, y, z, c], s_loc.at[0]
                ).start()
                col = pl.multiple_of(p * 512 + q * 128, 128)
                pltpu.make_async_copy(
                    w_d.at[b, :, pl.ds(col, 128)], WD.at[b, p, q, y, z, c], s_loc.at[1]
                ).start()
        return u

    lax.fori_loop(0, 4, fill, 0)
    for j in range(8):
        if j < 3:
            for q in range(4):
                pltpu.make_async_copy(
                    w_p.at[pl.ds(q * 16, 16), pl.ds(j * 128, 128)], WP.at[j, y, z, c, q], s_loc.at[2]
                ).start()
        else:
            pltpu.make_async_copy(
                w_p.at[pl.ds(pl.multiple_of(x * 16, 16), 16), pl.ds(j * 128, 128)],
                WP.at[j, y, z, c, x],
                s_loc.at[3],
            ).start()
    get_deter.start()

    iota = lax.broadcasted_iota(jnp.int32, (256, 128), 0)
    sel_t = jnp.concatenate(
        [jnp.where(iota == rows_t[i : i + 1, :], 1.0, 0.0) for i in range(2)], axis=1
    )
    sel = jnp.transpose(sel_t).astype(BF)
    picked = dot(stoch_t[...].astype(F32).astype(BF), sel_t.astype(BF))
    zs = [
        jnp.where(counts[...] > i, picked[:, 128 * i : 128 * i + 128], 64.0) for i in range(2)
    ]
    zs = jnp.concatenate(zs + [jnp.zeros((64, 128), F32)], axis=0)
    send_z[...] = jnp.transpose(zs).astype(jnp.int32).reshape(128, 1, 128)

    wait_bytes(WS.at[0, :, :, 0:2, 0, 0], s_loc.at[0])
    wait_bytes(WD.at[0, :, :, 0:2, 0, 0], s_loc.at[1])
    wait_bytes(WP.at[0:3, 0, 0, 0], s_loc.at[2])
    wait_bytes(WP.at[0:5, 0, 0, 0, 0], s_loc.at[3])

    def copy_to(ref, snd, rcv, to):
        return pltpu.make_async_remote_copy(
            src_ref=ref, dst_ref=ref, send_sem=snd, recv_sem=rcv, device_id=to, device_id_type=MESH
        )

    class Ring:
        def __init__(self, dim, part, half, snd, rcv, solo=False):
            self.dim, self.part, self.half, self.snd, self.rcv = dim, part, half, snd, rcv
            self.far = (2,) if solo else (2, 3)

        def at(self, step):
            return (pos[self.dim] + step + 4) % 4

        def make(self, ref, k):
            return copy_to(ref, self.snd(k), self.rcv.at[k], near(self.dim, 1 if k % 2 == 0 else -1))

        def start(self):
            for k in range(2):
                self.make(self.part(self.at(0)), k).start()

        def mid(self, then=None):
            for k in range(2):
                side = self.part(self.at(-1 if k == 0 else 1))
                self.make(side, k).wait_recv()
                if k + 2 in self.far:
                    self.make(self.half(self.at(-1 if k == 0 else 1), k), k + 2).start()
                if then is not None:
                    then(side)

        def end(self, then=None):
            for k in self.far:
                far = self.half(self.at(2), k - 2)
                self.make(far, k).wait_recv()
                if then is not None:
                    then(far)

    hs = (slice(0, 2), slice(2, 4))

    def rings(W, b, s):
        rows = 32 if s == 0 else 16

        def ring(n, dim, part, half, group, solo=False):
            return Ring(dim, part, half, lambda k: w_snd.at[b, s, group], w_rcv.at[b, s, n], solo)

        def split(ref, h):
            return ref if s == 1 else ref.at[pl.ds(16 * h, 16)]

        return {
            "ay": ring(0, "y", lambda i: W.at[b, 0, :, i, z, c], lambda i, h: W.at[b, 0, hs[h], i, z, c], 1),
            "by": ring(1, "y", lambda i: W.at[b, 1, x, i, z, c], lambda i, h: split(W.at[b, 1, x, i, z, c], h), 0, s == 1),
            "cz": ring(2, "z", lambda i: W.at[b, 2, x, y, i, c], lambda i, h: split(W.at[b, 2, x, y, i, c], h), 0, s == 1),
            "bz": ring(3, "z", lambda i: W.at[b, 1, x, :, i, c], lambda i, h: W.at[b, 1, x, hs[h], i, c], 1),
            "cx": ring(4, "x", lambda i: W.at[b, 2, i, y, :, c], lambda i, h: W.at[b, 2, i, y, hs[h], c], 1),
            "fz": ring(5, "z", lambda i: W.at[b, 0, :, :, i, c], lambda i, h: W.at[b, 0, hs[h], :, i, c], 2),
            "fx": ring(6, "x", lambda i: W.at[b, 1, i, :, :, c], lambda i, h: W.at[b, 1, i, hs[h], :, c], 2),
            "fy": ring(7, "y", lambda i: W.at[b, 2, :, i, :, c], lambda i, h: W.at[b, 2, hs[h], i, :, c], 2),
        }

    def rings_p():
        def ring(n, dim, part, half):
            return Ring(dim, part, half, lambda k: p_snd.at[n, k], p_rcv.at[n])

        return {
            "ay": ring(0, "y", lambda i: WP.at[0:3, i, z, c], lambda i, h: WP.at[0:3, i, z, c, hs[h]]),
            "by": ring(1, "y", lambda i: WP.at[3:6, i, z, c, x], lambda i, h: WP.at[3 + h : 4 + 2 * h, i, z, c, x]),
            "cz": ring(2, "z", lambda i: WP.at[6:8, y, i, c, x], lambda i, h: WP.at[6 + h : 7 + h, y, i, c, x]),
            "bz": ring(3, "z", lambda i: WP.at[3:6, :, i, c, x], lambda i, h: WP.at[3:6, hs[h], i, c, x]),
            "cx": ring(4, "x", lambda i: WP.at[6:8, y, :, c, i], lambda i, h: WP.at[6:8, y, hs[h], c, i]),
            "fz": ring(5, "z", lambda i: WP.at[0:3, :, i, c], lambda i, h: WP.at[0:3, hs[h], i, c]),
            "fx": ring(6, "x", lambda i: WP.at[3:6, :, :, c, i], lambda i, h: WP.at[3:6, hs[h], :, c, i]),
            "fy": ring(7, "y", lambda i: WP.at[6:8, i, :, c], lambda i, h: WP.at[6:8, i, hs[h], c]),
        }

    def over(k):
        def go(ref):
            copy_to(ref, d_snd.at[k], d_rcv.at[k], partner).start()

        return go

    def stage(n, b):
        if isinstance(b, int) and b == 4:
            sets = [(rings_p(), over(8))]
        else:
            sets = [(rings(WS, b, 0), over(2 * b)), (rings(WD, b, 1), over(2 * b + 1))]

        def each(names, what, hand=False):
            for name in names:
                for r, give in sets:
                    what(r[name], give if hand else None)

        def start(r, give):
            r.start()
            if give is not None:
                give(r.part(r.at(0)))

        if n == 1:
            each(("by", "cz", "ay"), start)
        elif n == 2:
            each(("by", "cz", "ay"), Ring.mid)
        elif n == 3:
            each(("by", "cz"), Ring.end)
            each(("bz", "cx"), start)
        elif n == 4:
            each(("bz", "cx"), Ring.mid)
            each(("ay",), Ring.end)
            each(("fz",), start, True)
        elif n == 5:
            each(("bz", "cx"), Ring.end)
            each(("fx", "fy"), start, True)
        elif n == 6:
            each(("fz", "fx", "fy"), Ring.mid, True)
        else:
            each(("fz", "fx", "fy"), Ring.end, True)

    def ready(b):
        wait_bytes(WS.at[b, :, :, :, :, 1 - c], d_rcv.at[2 * b])
        wait_bytes(WD.at[b, :, :, :, :, 1 - c], d_rcv.at[2 * b + 1])

    stage(1, 0)
    stage(1, 1)

    get_deter.wait()
    for k in range(8):
        lo = 512 * (k // 2) + 128 * (k % 2)
        parts = []
        for col in (lo, lo + 256):
            code = jnp.round(deter[:, col : col + 128] * SCALE)
            high = jnp.floor(code * (1.0 / 256.0))
            parts += [high.astype(BF), (code - high * 256.0).astype(BF)]
        got = dot(sel, jnp.concatenate(parts, axis=1))
        v0 = (got[:, 0:128] * 256.0 + got[:, 128:256]).astype(jnp.int32)
        v1 = (got[:, 256:384] * 256.0 + got[:, 384:512]).astype(jnp.int32)
        word = v1 * 65536 + (v0 + 32768)
        send[pl.ds(k, 128, stride=16), :] = word[0:128]
        send[pl.ds(8 + k, 128, stride=16), :] = word[128:256]
        if k == 4:
            stage(2, 0)
            stage(1, 2)

    stage(3, 0)
    stage(2, 1)

    def rows_of(n):
        return pl.ds(pl.multiple_of(n * 16, 16), 16)

    def a2a_start(i, u):
        r = i % 32
        tx, ty, tz, tc = (x + i // 32) % 4, (y + r // 8) % 4, (z + (r // 2) % 4) % 4, (c + r % 2) % 2
        to = dev(tx, ty, tz, tc)
        n = tx * 32 + ty * 8 + tz * 2 + tc
        pltpu.make_async_remote_copy(
            src_ref=send.at[rows_of(n), :], dst_ref=recv.at[rows_of(me), :],
            send_sem=s_snd.at[0], recv_sem=s_rcv.at[0], device_id=to, device_id_type=MESH,
        ).start()
        pltpu.make_async_remote_copy(
            src_ref=send_z.at[n], dst_ref=recv_z.at[me],
            send_sem=s_snd.at[1], recv_sem=s_rcv.at[1], device_id=to, device_id_type=MESH,
        ).start()
        return u

    lax.fori_loop(1, 128, a2a_start, 0)
    own = [
        pltpu.make_async_copy(send.at[rows_of(me), :], recv.at[rows_of(me), :], s_loc.at[4]),
        pltpu.make_async_copy(send_z.at[me], recv_z.at[me], s_loc.at[5]),
    ]
    for cp in own:
        cp.start()

    E = spread(32, 1024)
    cls = (lax.broadcasted_iota(jnp.int32, (256, 1024), 1) % 32).astype(F32)

    def one_hot(t):
        rep = dot(samps_t[t - 1].astype(F32).astype(BF), E, ((0,), (0,)))
        OH[t] = jnp.where(rep == cls, 1.0, 0.0).astype(BF)

    stage(4, 0)
    stage(3, 1)
    stage(2, 2)
    stage(1, 3)
    one_hot(1)
    ACT[...] = jnp.zeros_like(ACT)
    ACT[0 : act.shape[0], :] = act[...]
    stage(5, 0)
    stage(4, 1)
    stage(3, 2)
    stage(2, 3)
    stage(1, 4)
    one_hot(2)
    one_hot(3)
    stage(6, 0)
    stage(5, 1)
    stage(4, 2)
    stage(3, 3)
    stage(2, 4)

    wait_bytes(recv_z.at[pl.ds(0, 127)], s_rcv.at[1])
    wait_bytes(recv.at[pl.ds(0, 127 * 16), :], s_rcv.at[0])
    for cp in own:
        cp.wait()
    zv = recv_z[...].reshape(128, 128)
    zf[pl.ds(0, 128, stride=2), :] = zv
    zf[pl.ds(1, 128, stride=2), :] = pltpu.roll(zv, 96, 1)
    codes = zf[...].astype(F32)
    rep = dot(codes[:, 0:32].astype(BF), E)
    OH[0] = jnp.where(rep == cls, 1.0, 0.0).astype(BF)
    alive = jnp.where(codes < 32.0, 1.0, 0.0)
    lane0 = jnp.where(lax.broadcasted_iota(jnp.int32, (8, 128), 1) == 0, 1.0, 0.0).astype(BF)
    live_out[...] = dot(lane0, alive.astype(BF), ((1,), (1,)))
    live_col = alive[:, 0:1]
    for k in range(8):
        word = recv[pl.ds(k, 256, stride=8), :]
        v1 = lax.shift_right_arithmetic(word, 16)
        v0 = (word & 65535) - 32768
        b, e = k // 2, (k % 2) * 128
        H0[b, :, e : e + 128] = v0.astype(F32) * (1.0 / SCALE)
        H0[b, :, 256 + e : 384 + e] = v1.astype(F32) * (1.0 / SCALE)

    stage(7, 0)
    stage(6, 1)
    stage(5, 2)
    stage(4, 3)
    stage(3, 4)
    ready(0)

    def compute(b, u):
        def gate(p):
            def pre(t, u):
                rhs = jnp.concatenate([WS[b, p, q].reshape(1024, 128) for q in range(4)], axis=1)
                a_hot = jnp.where(
                    lax.broadcasted_iota(jnp.int32, (32, 256), 0) == acts_t[pl.ds(t, 1), :], 1.0, 0.0
                ).astype(BF)
                cols = pl.ds(pl.multiple_of(b * 1536 + p * 512, 512), 512)
                PRE[t, p] = dot(OH[t], rhs) + dot(a_hot, ACT[:, cols], ((0,), (0,)))
                return u

            lax.fori_loop(0, STEPS, pre, 0)

        gate(0)

        @pl.when(b < 2)
        def _():
            stage(6, b + 2)

        @pl.when(b == 2)
        def _():
            stage(6, 4)

        @pl.when(b == 0)
        def _():
            stage(5, 3)
            stage(4, 4)

        @pl.when(b == 1)
        def _():
            stage(5, 4)

        gate(1)

        @pl.when(b < 3)
        def _():
            stage(7, b + 1)

        @pl.when(b == 3)
        def _():
            stage(7, 4)

        gate(2)
        H[...] = H0[b]

        def step(t, u):
            h = H[...]
            low = h.astype(BF)

            def gates(p):
                rhs = jnp.concatenate([WD[b, p, q].reshape(512, 128) for q in range(4)], axis=1)
                return PRE[t, p] + dot(low, rhs)

            cand = jnp.tanh(sig(gates(0)) * gates(1))
            g = sig(gates(2) - 1.0)
            new = g * cand + (1.0 - g) * h
            H[...] = new
            ST[b, t] = (new * live_col).astype(BF)
            return u

        lax.fori_loop(0, STEPS, step, 0)
        pltpu.make_async_copy(ST.at[b], st_out.at[b], s_out.at[b]).start()

        @pl.when(b < 3)
        def _():
            ready(b + 1)

        return u

    lax.fori_loop(0, BLOCKS, compute, 0)
    wait_bytes(WP.at[:, :, :, 1 - c], d_rcv.at[8])
    out_p = pltpu.make_async_copy(WP, wp_out, s_out.at[4])
    out_p.start()
    wait_bytes(send.at[pl.ds(0, 127 * 16), :], s_snd.at[0])
    wait_bytes(send_z.at[pl.ds(0, 127)], s_snd.at[1])

    def drain(b, u):
        for s, W in enumerate((WS, WD)):
            wait_bytes(W.at[b, :, 0:2, 0, 0, 0], w_snd.at[b, s, 0])
            wait_bytes(W.at[b, :, 0:3, :, 0, 0], w_snd.at[b, s, 1])
            wait_bytes(W.at[b, :, 0:3, :, :, 0], w_snd.at[b, s, 2])
            wait_bytes(W.at[b, :, :, :, :, c], d_snd.at[2 * b + s])
        pltpu.make_async_copy(ST.at[b], st_out.at[b], s_out.at[b]).wait()
        return u

    lax.fori_loop(0, BLOCKS, drain, 0)
    for r in rings_p().values():
        for k in range(4):
            ref = r.part(r.at(0)) if k < 2 else r.half(r.at(-1 if k == 2 else 1), k - 2)
            r.make(ref, k).wait_send()
    wait_bytes(WP.at[:, :, :, c], d_snd.at[8])
    out_p.wait()


def prior_kernel(st, wp, live, samps_t, img, lp, stv, wpv, hot, scr, imgv, s_in, s_w, s_out):
    def part(s):
        return pl.ds(pl.multiple_of(s * 128, 128), 128)

    def get_w(b):
        return pltpu.make_async_copy(wp.at[:, b], wpv.at[:, b], s_w.at[b])

    def get_s(s):
        return pltpu.make_async_copy(st.at[:, :, part(s)], stv.at[:, :, part(s)], s_in.at[s])

    def put(s):
        return pltpu.make_async_copy(imgv.at[part(s)], img.at[part(s)], s_out.at[s])

    get_s(0).start()
    for b in range(BLOCKS):
        get_w(b).start()
    get_s(1).start()
    E = spread(32, 1024)
    cls = (lax.broadcasted_iota(jnp.int32, (256, 1024), 1) % 32).astype(F32)

    def hits(t, u):
        rep = dot(samps_t[t].astype(F32).astype(BF), E, ((0,), (0,)))
        hot[t] = jnp.where(rep == cls, 1.0, 0.0).astype(BF)
        return u

    lax.fori_loop(0, STEPS, hits, 0)

    def half(s, u):
        get_s(s).wait()

        def lay(b, u):
            for t in range(STEPS):
                scr[:, t, :] = stv[b, t, part(s)].astype(F32)
            cols = pl.ds(pl.multiple_of(b * 512, 512), 512)
            imgv[part(s), :, cols] = scr[...].astype(BF)
            return u

        lax.fori_loop(0, BLOCKS, lay, 0)
        put(s).start()

        @pl.when(s == 0)
        def _():
            for b in range(BLOCKS):
                get_w(b).wait()

        def step(t, u):
            low = jnp.concatenate([stv[b, t, part(s)] for b in range(BLOCKS)], axis=1)
            rhs = jnp.concatenate([wpv[j].reshape(2048, 128) for j in range(8)], axis=1)
            logits = dot(low, rhs)

            def grouped(v):
                hi = v.astype(BF)
                lo = (v - hi.astype(F32)).astype(BF)
                return dot(E, hi, ((1,), (1,))) + dot(E, lo, ((1,), (1,)))

            total = jnp.log(grouped(jnp.exp(logits)))
            hit = grouped(logits * hot[t, part(s)].astype(F32))
            lp[t, :, part(s)] = jnp.where(live[0:1, part(s)] > 0.0, hit - total, 0.0)
            return u

        lax.fori_loop(0, STEPS, step, 0)
        return u

    lax.fori_loop(0, 2, half, 0)
    put(0).wait()
    put(1).wait()


def on_device(deter, stoch, rows, counts, acts, samps, w_s, w_d, act, w_p):
    vmem = pl.BlockSpec(memory_space=pltpu.VMEM)
    hbm = pl.BlockSpec(memory_space=pl.ANY)
    dma = pltpu.SemaphoreType.DMA
    samps_t = samps.transpose(1, 2, 0)
    states, wp, live = pl.pallas_call(
        gru_kernel,
        name="gru",
        out_shape=(
            jax.ShapeDtypeStruct((4, 4, 256, 512), BF),
            jax.ShapeDtypeStruct((8, 4, 4, 2, 4, 16, 128), BF),
            jax.ShapeDtypeStruct((8, 256), F32),
        ),
        in_specs=[hbm] + [vmem] * 5 + [hbm, hbm, vmem, hbm],
        out_specs=(hbm, hbm, vmem),
        scratch_shapes=[
            pltpu.VMEM((256, 2048), F32),
            pltpu.VMEM((4, 3, 4, 4, 4, 2, 32, 128), BF),
            pltpu.VMEM((4, 3, 4, 4, 4, 2, 16, 128), BF),
            pltpu.VMEM((8, 4, 4, 2, 4, 16, 128), BF),
            pltpu.VMEM((2048, 128), jnp.int32),
            pltpu.VMEM((2048, 128), jnp.int32),
            pltpu.VMEM((128, 1, 128), jnp.int32),
            pltpu.VMEM((128, 1, 128), jnp.int32),
            pltpu.VMEM((256, 128), jnp.int32),
            pltpu.VMEM((4, 256, 512), F32),
            pltpu.VMEM((256, 512), F32),
            pltpu.VMEM((4, 256, 1024), BF),
            pltpu.VMEM((32, 6144), BF),
            pltpu.VMEM((4, 3, 256, 512), F32),
            pltpu.VMEM((4, 4, 256, 512), BF),
            dma((7,)), dma((2,)), dma((2,)),
            dma((4, 2, 3)), dma((4, 2, 8, 4)),
            dma((8, 4)), dma((8, 4)),
            dma((9,)), dma((9,)), dma((5,)),
        ],
        compiler_params=pltpu.CompilerParams(
            has_side_effects=True, vmem_limit_bytes=60 * 1024 * 1024
        ),
    )(deter, stoch.T, rows.T, counts, acts.T, samps_t, w_s, w_d, act, w_p)
    imagined, logp = pl.pallas_call(
        prior_kernel,
        name="prior",
        out_shape=(
            jax.ShapeDtypeStruct((256, 4, 2048), BF),
            jax.ShapeDtypeStruct((4, 32, 256), F32),
        ),
        in_specs=[hbm, hbm, vmem, vmem],
        out_specs=(hbm, vmem),
        scratch_shapes=[
            pltpu.VMEM((4, 4, 256, 512), BF),
            pltpu.VMEM((8, 4, 4, 2, 4, 16, 128), BF),
            pltpu.VMEM((4, 256, 1024), BF),
            pltpu.VMEM((128, 4, 512), F32),
            pltpu.VMEM((256, 4, 2048), BF),
            dma((2,)), dma((4,)), dma((2,)),
        ],
        compiler_params=pltpu.CompilerParams(vmem_limit_bytes=60 * 1024 * 1024),
    )(states, wp, live, samps_t)
    return (imagined, logp.transpose(2, 0, 1))


def solution(mesh):
    in_specs = (
        P(("gx", "gy"), None),
        P(("gx", "gy"), None),
        P(("gx", "gy"), None),
        P(("gx", "gy"), None),
        P(("gx", "gy"), None),
        P(("gx", "gy"), None, None),
        P("gy", None),
        P(None, "gy", None),
        P(),
        P("gy", None),
    )
    out_specs = (P(("gx", "gy"), None, None), P(("gx", "gy"), None, None))
    return jax.shard_map(
        on_device, mesh=mesh, in_specs=in_specs, out_specs=out_specs, check_vma=False
    )
```

```python
import functools

import jax
import jax.numpy as jnp
from jax import lax
from jax.experimental import pallas as pl
from jax.experimental.pallas import tpu as pltpu
from jax.sharding import PartitionSpec as P

STEPS = 4
BLOCKS = 4
BF = jnp.bfloat16
F32 = jnp.float32
MESH = pl.DeviceIdType.MESH
SCALE = 32767.0


def dot(a, b, dims=((1,), (0,))):
    return lax.dot_general(a, b, (dims, ((), ())), preferred_element_type=F32)


def spread(rows, lanes):
    g = lax.broadcasted_iota(jnp.int32, (rows, lanes), 0)
    k = lax.broadcasted_iota(jnp.int32, (rows, lanes), 1)
    return jnp.where((k >= g * 32) & (k < g * 32 + 32), 1.0, 0.0).astype(BF)


def sig(v):
    return 0.5 * jnp.tanh(0.5 * v) + 0.5


def gru_kernel(
    deter_h, stoch_t, rows_t, counts, acts_t, samps_t, w_s, w_d, act, w_p,
    st_out, wp_out, live_out,
    deter, WS, WD, WP, send, recv, send_z, recv_z, zf, H0, H, OH, ACT, AH, PRE, ST,
    s_loc, s_snd, s_rcv, w_snd, w_rcv, p_snd, p_rcv, d_snd, d_rcv, s_out,
):
    x = lax.axis_index("gx")
    gy = lax.axis_index("gy")
    y, z, c = gy // 8, (gy // 2) % 4, gy % 2
    me = x * 32 + gy

    def dev(tx, ty, tz, tc):
        return (tx, ty * 8 + tz * 2 + tc)

    def near(dim, step):
        s = (step + 4) % 4
        if dim == "x":
            return dev((x + s) % 4, y, z, c)
        if dim == "y":
            return dev(x, (y + s) % 4, z, c)
        return dev(x, y, (z + s) % 4, c)

    pos = {"x": x, "y": y, "z": z}
    partner = dev(x, y, z, 1 - c)

    def wait_bytes(ref, sem):
        pltpu.make_async_copy(ref, ref, sem).wait()

    barrier = pltpu.get_barrier_semaphore()

    xs, ys, zs = ([(v + i) % 4 for i in range(4)] for v in (x, y, z))
    y8, z2, cs = [v * 8 for v in ys], [v * 2 for v in zs], [c, 1 - c]

    def peers(*dxs):
        for dx in dxs:
            for dy in range(4):
                for dz in range(4):
                    for dc in range(2):
                        if dx + dy + dz + dc > 0:
                            g = y8[dy] + (z2[dz] + cs[dc])
                            yield (xs[dx], g), xs[dx] * 32 + g

    for to, _ in peers(0, 1, 2, 3):
        pl.semaphore_signal(barrier, inc=1, device_id=to, device_id_type=MESH)
    get_deter = pltpu.make_async_copy(deter_h, deter, s_loc.at[6])

    def fill(b, u):
        for p in range(3):
            for q in range(4) if p == 0 else (x,):
                col = pl.multiple_of(b * 1536 + p * 512 + q * 128, 128)
                pltpu.make_async_copy(
                    w_s.at[:, pl.ds(col, 128)], WS.at[b, p, q, y, z, c], s_loc.at[0]
                ).start()
                col = pl.multiple_of(p * 512 + q * 128, 128)
                pltpu.make_async_copy(
                    w_d.at[b, :, pl.ds(col, 128)], WD.at[b, p, q, y, z, c], s_loc.at[1]
                ).start()
        return u

    lax.fori_loop(0, 4, fill, 0)
    for j in range(8):
        if j < 3:
            for q in range(4):
                pltpu.make_async_copy(
                    w_p.at[pl.ds(q * 16, 16), pl.ds(j * 128, 128)], WP.at[j, y, z, c, q], s_loc.at[2]
                ).start()
        else:
            pltpu.make_async_copy(
                w_p.at[pl.ds(pl.multiple_of(x * 16, 16), 16), pl.ds(j * 128, 128)],
                WP.at[j, y, z, c, x],
                s_loc.at[3],
            ).start()
    get_deter.start()

    iota = lax.broadcasted_iota(jnp.int32, (256, 128), 0)
    sel_t = jnp.concatenate(
        [jnp.where(iota == rows_t[i : i + 1, :], 1.0, 0.0) for i in range(2)], axis=1
    )
    sel = jnp.transpose(sel_t).astype(BF)
    picked = dot(stoch_t[...].astype(F32).astype(BF), sel_t.astype(BF))
    zv = [
        jnp.where(counts[...] > i, picked[:, 128 * i : 128 * i + 128], 64.0) for i in range(2)
    ]
    zv = jnp.concatenate(zv + [jnp.zeros((64, 128), F32)], axis=0)
    send_z[...] = jnp.transpose(zv).astype(jnp.int32).reshape(128, 1, 128)

    wait_bytes(WS.at[0, :, :, 0:2, 0, 0], s_loc.at[0])
    wait_bytes(WD.at[0, :, :, 0:2, 0, 0], s_loc.at[1])
    wait_bytes(WP.at[0:3, 0, 0, 0], s_loc.at[2])
    wait_bytes(WP.at[0:5, 0, 0, 0, 0], s_loc.at[3])

    pl.semaphore_wait(barrier, 127)

    def copy_to(ref, snd, rcv, to):
        return pltpu.make_async_remote_copy(
            src_ref=ref, dst_ref=ref, send_sem=snd, recv_sem=rcv, device_id=to, device_id_type=MESH
        )

    class Ring:
        def __init__(self, dim, sets, snd, rcv, sides, far):
            self.dim, self.sets, self.snd, self.rcv = dim, sets, snd, rcv
            self.sides, self.far = sides, far

        def at(self, step):
            return (pos[self.dim] + step + 4) % 4

        def send(self, ref, k, stage):
            copy_to(ref, self.snd, self.rcv.at[stage], near(self.dim, 1 if k == 0 else -1)).start()

        def start(self, hand):
            for part, half in self.sets:
                for k in range(2):
                    self.send(part(self.at(0)), k, 0)
            if hand:
                for part, half in self.sets:
                    hand(part(self.at(0)))

        def mid(self, hand):
            wait_bytes(self.sides, self.rcv.at[0])
            for part, half in self.sets:
                for k in range(2):
                    ref = half(self.at(-1 if k == 0 else 1), k)
                    if ref is not None:
                        self.send(ref, k, 1)
            if hand:
                for part, half in self.sets:
                    for k in (-1, 1):
                        hand(part(self.at(k)))

        def end(self, hand):
            wait_bytes(self.far, self.rcv.at[1])
            if hand:
                for part, half in self.sets:
                    hand(part(self.at(2)))

    hs = (slice(0, 2), slice(2, 4))

    def rings(b):
        def ring(n, dim, part, half, group, size):
            sets = [(functools.partial(part, W), functools.partial(half, W)) for W in (WS, WD)]
            spare = {1: (0, 0, 0), 4: (slice(None), 0, 0), 16: (slice(None), slice(None), 0)}[size]
            return Ring(
                dim, sets, w_snd.at[b, group], w_rcv.at[b, n],
                WD.at[(slice(0, 2), slice(0, 3)) + spare + (0,)], WD.at[(0, slice(0, 3)) + spare + (0,)],
            )

        def split(W, ref, h):
            if W is WS:
                return ref.at[pl.ds(16 * h, 16)]
            return ref if h == 0 else None

        return {
            "ay": ring(0, "y", lambda W, i: W.at[b, 0, :, i, z, c], lambda W, i, h: W.at[b, 0, hs[h], i, z, c], 1, 4),
            "by": ring(1, "y", lambda W, i: W.at[b, 1, x, i, z, c], lambda W, i, h: split(W, W.at[b, 1, x, i, z, c], h), 0, 1),
            "cz": ring(2, "z", lambda W, i: W.at[b, 2, x, y, i, c], lambda W, i, h: split(W, W.at[b, 2, x, y, i, c], h), 0, 1),
            "bz": ring(3, "z", lambda W, i: W.at[b, 1, x, :, i, c], lambda W, i, h: W.at[b, 1, x, hs[h], i, c], 1, 4),
            "cx": ring(4, "x", lambda W, i: W.at[b, 2, i, y, :, c], lambda W, i, h: W.at[b, 2, i, y, hs[h], c], 1, 4),
            "fz": ring(5, "z", lambda W, i: W.at[b, 0, :, :, i, c], lambda W, i, h: W.at[b, 0, hs[h], :, i, c], 2, 16),
            "fx": ring(6, "x", lambda W, i: W.at[b, 1, i, :, :, c], lambda W, i, h: W.at[b, 1, i, hs[h], :, c], 2, 16),
            "fy": ring(7, "y", lambda W, i: W.at[b, 2, :, i, :, c], lambda W, i, h: W.at[b, 2, hs[h], i, :, c], 2, 16),
        }

    def rings_p():
        def ring(n, dim, part, half, group, sides, far):
            return Ring(dim, [(part, half)], p_snd.at[group], p_rcv.at[n], sides, far)

        return {
            "ay": ring(0, "y", lambda i: WP.at[0:3, i, z, c], lambda i, h: WP.at[0:3, i, z, c, hs[h]], 0, WP.at[0:3, :, 0, :, 0], WP.at[0:3, :, 0, 0, 0]),
            "by": ring(1, "y", lambda i: WP.at[3:6, i, z, c, x], lambda i, h: WP.at[3 + h : 4 + 2 * h, i, z, c, x], 1, WP.at[0:6, 0, 0, 0, 0], WP.at[0:3, 0, 0, 0, 0]),
            "cz": ring(2, "z", lambda i: WP.at[6:8, y, i, c, x], lambda i, h: WP.at[6 + h : 7 + h, y, i, c, x], 1, WP.at[0:4, 0, 0, 0, 0], WP.at[0:2, 0, 0, 0, 0]),
            "bz": ring(3, "z", lambda i: WP.at[3:6, :, i, c, x], lambda i, h: WP.at[3:6, hs[h], i, c, x], 0, WP.at[0:3, :, 0, :, 0], WP.at[0:3, :, 0, 0, 0]),
            "cx": ring(4, "x", lambda i: WP.at[6:8, y, :, c, i], lambda i, h: WP.at[6:8, y, hs[h], c, i], 2, WP.at[0:4, :, 0, 0, 0], WP.at[0:2, :, 0, 0, 0]),
            "fz": ring(5, "z", lambda i: WP.at[0:3, :, i, c], lambda i, h: WP.at[0:3, hs[h], i, c], 3, WP.at[0:3, :, :, :, 0], WP.at[0:3, :, :, 0, 0]),
            "fx": ring(6, "x", lambda i: WP.at[3:6, :, :, c, i], lambda i, h: WP.at[3:6, hs[h], :, c, i], 3, WP.at[0:3, :, :, :, 0], WP.at[0:3, :, :, 0, 0]),
            "fy": ring(7, "y", lambda i: WP.at[6:8, i, :, c], lambda i, h: WP.at[6:8, i, hs[h], c], 4, WP.at[0:2, :, :, :, 0], WP.at[0:2, :, :, 0, 0]),
        }

    def over(k):
        def go(ref):
            copy_to(ref, d_snd.at[k], d_rcv.at[k], partner).start()

        return go

    def stage(n, b):
        if isinstance(b, int) and b == 4:
            r, give = rings_p(), over(4)
        else:
            r, give = rings(b), over(b)

        def each(names, what, hand=None):
            for name in names:
                what(r[name], hand)

        if n == 1:
            each(("by", "cz", "ay"), Ring.start)
        elif n == 2:
            each(("by", "cz", "ay"), Ring.mid)
        elif n == 3:
            each(("by", "cz"), Ring.end)
            each(("bz", "cx"), Ring.start)
        elif n == 4:
            each(("bz", "cx"), Ring.mid)
            each(("ay",), Ring.end)
        elif n == 5:
            each(("bz", "cx"), Ring.end)
            each(("fz", "fx", "fy"), Ring.start, give)
        elif n == 6:
            each(("fz", "fx", "fy"), Ring.mid, give)
        else:
            each(("fz", "fx", "fy"), Ring.end, give)

    def ready(b):
        wait_bytes(WD.at[0:3, :, :, :, :, 0], d_rcv.at[b])

    stage(1, 0)
    stage(1, 1)
    for to, n in peers(0, 1, 2, 3):
        pltpu.make_async_remote_copy(
            src_ref=send_z.at[n], dst_ref=recv_z.at[me],
            send_sem=s_snd.at[1], recv_sem=s_rcv.at[1], device_id=to, device_id_type=MESH,
        ).start()

    get_deter.wait()
    for k in range(8):
        lo = 512 * (k // 2) + 128 * (k % 2)
        parts = []
        for col in (lo, lo + 256):
            code = jnp.round(deter[:, col : col + 128] * SCALE)
            high = jnp.floor(code * (1.0 / 256.0))
            parts += [high.astype(BF), (code - high * 256.0).astype(BF)]
        got = dot(sel, jnp.concatenate(parts, axis=1))
        v0 = (got[:, 0:128] * 256.0 + got[:, 128:256]).astype(jnp.int32)
        v1 = (got[:, 256:384] * 256.0 + got[:, 384:512]).astype(jnp.int32)
        word = v1 * 65536 + (v0 + 32768)
        send[pl.ds(k, 128, stride=16), :] = word[0:128]
        send[pl.ds(8 + k, 128, stride=16), :] = word[128:256]
        if k == 2:
            stage(2, 0)

    def rows_of(n):
        return pl.ds(pl.multiple_of(n * 16, 16), 16)

    def send_rows(dx):
        for to, n in peers(dx):
            pltpu.make_async_remote_copy(
                src_ref=send.at[rows_of(n), :], dst_ref=recv.at[rows_of(me), :],
                send_sem=s_snd.at[0], recv_sem=s_rcv.at[0], device_id=to, device_id_type=MESH,
            ).start()

    stage(3, 0)
    send_rows(0)
    stage(2, 1)
    stage(1, 2)
    own = [
        pltpu.make_async_copy(send.at[rows_of(me), :], recv.at[rows_of(me), :], s_loc.at[4]),
        pltpu.make_async_copy(send_z.at[me], recv_z.at[me], s_loc.at[5]),
    ]
    for cp in own:
        cp.start()

    E = spread(32, 1024)
    cls = (lax.broadcasted_iota(jnp.int32, (256, 1024), 1) % 32).astype(F32)

    def one_hot(t):
        rep = dot(samps_t[t - 1].astype(F32).astype(BF), E, ((0,), (0,)))
        OH[256 * t : 256 * t + 256, :] = jnp.where(rep == cls, 1.0, 0.0).astype(BF)

    def act_terms(b):
        def piece(n, u):
            p, e = n // 2, n % 2
            cols = pl.ds(pl.multiple_of(b * 1536 + n * 256, 256), 256)
            PRE[b, p, :, pl.ds(pl.multiple_of(e * 256, 256), 256)] = dot(AH[...], ACT[:, cols])
            return u

        lax.fori_loop(0, 6, piece, 0)

    one_hot(1)
    one_hot(2)
    stage(4, 0)
    stage(3, 1)
    send_rows(1)
    stage(2, 2)
    one_hot(3)
    ACT[...] = jnp.zeros_like(ACT)
    ACT[0 : act.shape[0], :] = act[...]
    which = lax.broadcasted_iota(jnp.int32, (32, 256), 0)
    for t in range(STEPS):
        a_hot = jnp.where(which == acts_t[t : t + 1, :], 1.0, 0.0)
        AH[256 * t : 256 * t + 256, :] = jnp.transpose(a_hot).astype(BF)
    stage(5, 0)
    stage(1, 3)
    act_terms(0)
    stage(4, 1)
    stage(3, 2)
    send_rows(2)
    act_terms(1)
    act_terms(2)
    act_terms(3)
    stage(6, 0)
    send_rows(3)
    stage(5, 1)
    stage(2, 3)

    wait_bytes(recv_z.at[pl.ds(0, 127)], s_rcv.at[1])
    own[1].wait()
    zv = recv_z[...].reshape(128, 128)
    zf[pl.ds(0, 128, stride=2), :] = zv
    zf[pl.ds(1, 128, stride=2), :] = pltpu.roll(zv, 96, 1)
    codes = zf[...].astype(F32)
    rep = dot(codes[:, 0:32].astype(BF), E)
    OH[0:256, :] = jnp.where(rep == cls, 1.0, 0.0).astype(BF)
    alive = jnp.where(codes < 32.0, 1.0, 0.0)
    lane0 = jnp.where(lax.broadcasted_iota(jnp.int32, (8, 128), 1) == 0, 1.0, 0.0).astype(BF)
    live_out[...] = dot(lane0, alive.astype(BF), ((1,), (1,)))
    live_col = alive[:, 0:1]
    stage(7, 0)
    ready(0)

    def start_rows():
        wait_bytes(recv.at[pl.ds(0, 127 * 16), :], s_rcv.at[0])
        own[0].wait()
        for k in range(8):
            word = recv[pl.ds(k, 256, stride=8), :]
            v1 = lax.shift_right_arithmetic(word, 16)
            v0 = (word & 65535) - 32768
            b, e = k // 2, (k % 2) * 128
            H0[b, :, e : e + 128] = v0.astype(F32) * (1.0 / SCALE)
            H0[b, :, 256 + e : 384 + e] = v1.astype(F32) * (1.0 / SCALE)

    def put_states(b):
        return pltpu.make_async_copy(ST.at[b % 2], st_out.at[b], s_out.at[b])

    def compute(b, u):
        def gate(p):
            def piece(e, u):
                rhs = jnp.concatenate(
                    [WS[b, p, 2 * e + i].reshape(1024, 128) for i in range(2)], axis=1
                )
                cols = pl.ds(pl.multiple_of(e * 256, 256), 256)
                PRE[b, p, :, cols] = PRE[b, p, :, cols] + dot(OH[...], rhs)
                return u

            lax.fori_loop(0, 2, piece, 0)

        def also(plan):
            for when, stages in plan.items():

                @pl.when(b == when)
                def _():
                    for n, k in stages:
                        stage(n, k)

        gate(0)
        also({0: ((4, 2), (1, 4)), 1: ((6, 2), (3, 4)), 2: ((6, 3),), 3: ((6, 4),)})
        gate(1)
        also({0: ((6, 1), (3, 3)), 1: ((5, 3),), 2: ((5, 4),)})
        gate(2)

        @pl.when(b == 0)
        def _():
            stage(5, 2)
            start_rows()

        H[...] = H0[b]

        @pl.when(b >= 2)
        def _():
            put_states(b - 2).wait()

        def step(t, u):
            h = H[...]
            low = h.astype(BF)
            rows = pl.ds(pl.multiple_of(t * 256, 256), 256)

            def gates(p):
                rhs = jnp.concatenate([WD[b, p, q].reshape(512, 128) for q in range(4)], axis=1)
                return PRE[b, p, rows, :] + dot(low, rhs)

            cand = jnp.tanh(sig(gates(0)) * gates(1))
            g = sig(gates(2) - 1.0)
            new = g * cand + (1.0 - g) * h
            H[...] = new
            ST[b % 2, t] = (new * live_col).astype(BF)
            return u

        lax.fori_loop(0, 2, step, 0)

        @pl.when(b < 3)
        def _():
            stage(7, b + 1)

        also({0: ((2, 4),), 3: ((7, 4),)})
        lax.fori_loop(2, STEPS, step, 0)
        put_states(b).start()

        also({0: ((4, 3),), 1: ((4, 4),)})

        @pl.when(b < 3)
        def _():
            ready(b + 1)

        return u

    lax.fori_loop(0, BLOCKS, compute, 0)
    wait_bytes(WP.at[:, :, :, 0], d_rcv.at[4])
    out_p = pltpu.make_async_copy(WP, wp_out, s_out.at[4])
    out_p.start()
    wait_bytes(send.at[pl.ds(0, 127 * 16), :], s_snd.at[0])
    wait_bytes(send_z.at[pl.ds(0, 127)], s_snd.at[1])

    def drain(b, u):
        wait_bytes(WD.at[0, :, 0:3, 0:2, 0, 0], w_snd.at[b, 0])
        wait_bytes(WD.at[0, :, 0:3, 0:3, :, 0], w_snd.at[b, 1])
        wait_bytes(WD.at[0:2, :, 0:3, :, 0:3, :], w_snd.at[b, 2])
        wait_bytes(WD.at[0:3, :, :, :, :, 0], d_snd.at[b])

        @pl.when(b >= 2)
        def _():
            put_states(b).wait()

        return u

    lax.fori_loop(0, BLOCKS, drain, 0)
    wait_bytes(WP.at[0:3, :, 0:3, :, 0], p_snd.at[0])
    wait_bytes(WP.at[0:5, 0:3, 0, 0, 0], p_snd.at[1])
    wait_bytes(WP.at[0:3, :, 0, :, 0], p_snd.at[2])
    wait_bytes(WP.at[0:3, :, :, :, 0:3], p_snd.at[3])
    wait_bytes(WP.at[0:3, :, :, :, 0], p_snd.at[4])
    wait_bytes(WP.at[:, :, :, 0], d_snd.at[4])
    out_p.wait()


def prior_kernel(st, wp, live, samps_t, img, lp, stv, wpv, hot, scr, imgv, s_in, s_w, s_out):
    def part(s):
        return pl.ds(pl.multiple_of(s * 128, 128), 128)

    def get_w(n):
        return pltpu.make_async_copy(wp.at[pl.ds(2 * n, 2)], wpv.at[pl.ds(2 * n, 2)], s_w.at[n])

    def get_s(s):
        return pltpu.make_async_copy(st.at[:, :, part(s)], stv.at[:, :, part(s)], s_in.at[s])

    def put(s):
        return pltpu.make_async_copy(imgv.at[part(s)], img.at[part(s)], s_out.at[s])

    get_s(0).start()
    for n in range(4):
        get_w(n).start()
    get_s(1).start()
    E = spread(32, 1024)
    E8 = spread(8, 256)
    cls = (lax.broadcasted_iota(jnp.int32, (256, 1024), 1) % 32).astype(F32)

    def hits(t, u):
        rep = dot(samps_t[t].astype(F32).astype(BF), E, ((0,), (0,)))
        hot[t] = jnp.where(rep == cls, 1.0, 0.0).astype(BF)
        return u

    lax.fori_loop(0, STEPS, hits, 0)

    def half(s, u):
        get_s(s).wait()

        def columns(n, u):
            @pl.when(s == 0)
            def _():
                get_w(n).wait()

            low = jnp.concatenate([stv[b, :, part(s)].reshape(512, 512) for b in range(BLOCKS)], axis=1)
            rhs = jnp.concatenate([wpv[2 * n + i].reshape(2048, 128) for i in range(2)], axis=1)
            logits = dot(low, rhs)
            for t in range(STEPS):
                scr[:, t, :] = stv[n, t, part(s)].astype(F32)
            imgv[part(s), :, pl.ds(pl.multiple_of(n * 512, 512), 512)] = scr[...].astype(BF)

            def grouped(v):
                hi = v.astype(BF)
                lo = (v - hi.astype(F32)).astype(BF)
                return dot(E8, hi, ((1,), (1,))) + dot(E8, lo, ((1,), (1,)))

            cols = pl.ds(pl.multiple_of(n * 256, 256), 256)
            total = jnp.log(grouped(jnp.exp(logits)))
            hit = grouped(logits * hot[:, part(s), cols].reshape(512, 256).astype(F32))
            value = hit - total
            for t in range(STEPS):
                lp[t, pl.ds(pl.multiple_of(n * 8, 8), 8), part(s)] = jnp.where(
                    live[:, part(s)] > 0.0, value[:, 128 * t : 128 * t + 128], 0.0
                )
            return u

        lax.fori_loop(0, 4, columns, 0)
        put(s).start()
        return u

    lax.fori_loop(0, 2, half, 0)
    put(0).wait()
    put(1).wait()


def on_device(deter, stoch, rows, counts, acts, samps, w_s, w_d, act, w_p):
    vmem = pl.BlockSpec(memory_space=pltpu.VMEM)
    hbm = pl.BlockSpec(memory_space=pl.ANY)
    dma = pltpu.SemaphoreType.DMA
    samps_t = samps.transpose(1, 2, 0)
    states, wp, live = pl.pallas_call(
        gru_kernel,
        name="gru",
        out_shape=(
            jax.ShapeDtypeStruct((4, 4, 256, 512), BF),
            jax.ShapeDtypeStruct((8, 4, 4, 2, 4, 16, 128), BF),
            jax.ShapeDtypeStruct((8, 256), F32),
        ),
        in_specs=[hbm] + [vmem] * 5 + [hbm, hbm, vmem, hbm],
        out_specs=(hbm, hbm, vmem),
        scratch_shapes=[
            pltpu.VMEM((256, 2048), F32),
            pltpu.VMEM((4, 3, 4, 4, 4, 2, 32, 128), BF),
            pltpu.VMEM((4, 3, 4, 4, 4, 2, 16, 128), BF),
            pltpu.VMEM((8, 4, 4, 2, 4, 16, 128), BF),
            pltpu.VMEM((2048, 128), jnp.int32),
            pltpu.VMEM((2048, 128), jnp.int32),
            pltpu.VMEM((128, 1, 128), jnp.int32),
            pltpu.VMEM((128, 1, 128), jnp.int32),
            pltpu.VMEM((256, 128), jnp.int32),
            pltpu.VMEM((4, 256, 512), F32),
            pltpu.VMEM((256, 512), F32),
            pltpu.VMEM((1024, 1024), BF),
            pltpu.VMEM((32, 6144), BF),
            pltpu.VMEM((1024, 32), BF),
            pltpu.VMEM((4, 3, 1024, 512), F32),
            pltpu.VMEM((2, 4, 256, 512), BF),
            dma((7,)), dma((2,)), dma((2,)),
            dma((4, 3)), dma((4, 8, 2)),
            dma((5,)), dma((8, 2)),
            dma((5,)), dma((5,)), dma((5,)),
        ],
        compiler_params=pltpu.CompilerParams(
            collective_id=0, has_side_effects=True, vmem_limit_bytes=63 * 1024 * 1024
        ),
    )(deter, stoch.T, rows.T, counts, acts.T, samps_t, w_s, w_d, act, w_p)
    imagined, logp = pl.pallas_call(
        prior_kernel,
        name="prior",
        out_shape=(
            jax.ShapeDtypeStruct((256, 4, 2048), BF),
            jax.ShapeDtypeStruct((4, 32, 256), F32),
        ),
        in_specs=[hbm, hbm, vmem, vmem],
        out_specs=(hbm, vmem),
        scratch_shapes=[
            pltpu.VMEM((4, 4, 256, 512), BF),
            pltpu.VMEM((8, 4, 4, 2, 4, 16, 128), BF),
            pltpu.VMEM((4, 256, 1024), BF),
            pltpu.VMEM((128, 4, 512), F32),
            pltpu.VMEM((256, 4, 2048), BF),
            dma((2,)), dma((4,)), dma((2,)),
        ],
        compiler_params=pltpu.CompilerParams(vmem_limit_bytes=60 * 1024 * 1024),
    )(states, wp, live, samps_t)
    return (imagined, logp.transpose(2, 0, 1))


def solution(mesh):
    in_specs = (
        P(("gx", "gy"), None),
        P(("gx", "gy"), None),
        P(("gx", "gy"), None),
        P(("gx", "gy"), None),
        P(("gx", "gy"), None),
        P(("gx", "gy"), None, None),
        P("gy", None),
        P(None, "gy", None),
        P(),
        P("gy", None),
    )
    out_specs = (P(("gx", "gy"), None, None), P(("gx", "gy"), None, None))
    return jax.shard_map(
        on_device, mesh=mesh, in_specs=in_specs, out_specs=out_specs, check_vma=False
    )
```

```python
import functools

import jax
import jax.numpy as jnp
from jax import lax
from jax.experimental import pallas as pl
from jax.experimental.pallas import tpu as pltpu
from jax.sharding import PartitionSpec as P

STEPS = 4
BLOCKS = 4
BF = jnp.bfloat16
F32 = jnp.float32
MESH = pl.DeviceIdType.MESH
SCALE = 32767.0


def dot(a, b, dims=((1,), (0,))):
    return lax.dot_general(a, b, (dims, ((), ())), preferred_element_type=F32)


def spread(rows, lanes):
    g = lax.broadcasted_iota(jnp.int32, (rows, lanes), 0)
    k = lax.broadcasted_iota(jnp.int32, (rows, lanes), 1)
    return jnp.where((k >= g * 32) & (k < g * 32 + 32), 1.0, 0.0).astype(BF)


def sig(v):
    return 0.5 * jnp.tanh(0.5 * v) + 0.5


def gru_kernel(
    deter_h, stoch_t, rows_t, counts, acts_t, samps_t, w_s, w_d, act, w_p,
    st_out, wp_out, live_out,
    deter, WS, WD, WP, send, recv, send_z, recv_z, zf, H0, H, OH, ACT, AH, PRE, ST,
    s_loc, s_snd, s_rcv, w_snd, w_rcv, p_snd, p_rcv, d_snd, d_rcv, s_out,
):
    x = lax.axis_index("gx")
    gy = lax.axis_index("gy")
    y, z, c = gy // 8, (gy // 2) % 4, gy % 2
    me = x * 32 + gy

    def dev(tx, ty, tz, tc):
        return (tx, ty * 8 + tz * 2 + tc)

    def near(dim, step):
        s = (step + 4) % 4
        if dim == "x":
            return dev((x + s) % 4, y, z, c)
        if dim == "y":
            return dev(x, (y + s) % 4, z, c)
        return dev(x, y, (z + s) % 4, c)

    pos = {"x": x, "y": y, "z": z}
    partner = dev(x, y, z, 1 - c)

    def wait_bytes(ref, sem):
        pltpu.make_async_copy(ref, ref, sem).wait()

    barrier = pltpu.get_barrier_semaphore()

    xs, ys, zs = ([(v + i) % 4 for i in range(4)] for v in (x, y, z))
    y8, z2, cs = [v * 8 for v in ys], [v * 2 for v in zs], [c, 1 - c]

    def peers(*groups):
        for dx in range(4):
            for dy in range(4):
                for dz in range(4):
                    for dc in range(2):
                        if dx + dy + dz + dc > 0 and (dx + dy + dz) % 4 in groups:
                            g = y8[dy] + (z2[dz] + cs[dc])
                            yield (xs[dx], g), xs[dx] * 32 + g

    for to, _ in reversed(list(peers(0, 1, 2, 3))):
        pl.semaphore_signal(barrier, inc=1, device_id=to, device_id_type=MESH)
    get_deter = pltpu.make_async_copy(deter_h, deter, s_loc.at[6])

    def fill(b, u):
        for p in range(3):
            for q in range(4) if p == 0 else (x,):
                col = pl.multiple_of(b * 1536 + p * 512 + q * 128, 128)
                pltpu.make_async_copy(
                    w_s.at[:, pl.ds(col, 128)], WS.at[b, p, q, y, z, c], s_loc.at[0]
                ).start()
                col = pl.multiple_of(p * 512 + q * 128, 128)
                pltpu.make_async_copy(
                    w_d.at[b, :, pl.ds(col, 128)], WD.at[b, p, q, y, z, c], s_loc.at[1]
                ).start()
        return u

    lax.fori_loop(0, 4, fill, 0)
    for j in range(8):
        if j < 3:
            for q in range(4):
                pltpu.make_async_copy(
                    w_p.at[pl.ds(q * 16, 16), pl.ds(j * 128, 128)], WP.at[j, y, z, c, q], s_loc.at[2]
                ).start()
        else:
            pltpu.make_async_copy(
                w_p.at[pl.ds(pl.multiple_of(x * 16, 16), 16), pl.ds(j * 128, 128)],
                WP.at[j, y, z, c, x],
                s_loc.at[3],
            ).start()
    get_deter.start()

    iota = lax.broadcasted_iota(jnp.int32, (256, 128), 0)
    sel_t = jnp.concatenate(
        [jnp.where(iota == rows_t[i : i + 1, :], 1.0, 0.0) for i in range(2)], axis=1
    )
    sel = jnp.transpose(sel_t).astype(BF)
    picked = dot(stoch_t[...].astype(F32).astype(BF), sel_t.astype(BF))
    zv = [
        jnp.where(counts[...] > i, picked[:, 128 * i : 128 * i + 128], 64.0) for i in range(2)
    ]
    zv = jnp.concatenate(zv + [jnp.zeros((64, 128), F32)], axis=0)
    send_z[...] = jnp.transpose(zv).astype(jnp.int32).reshape(128, 1, 128)

    wait_bytes(WS.at[0, :, :, 0:2, 0, 0], s_loc.at[0])
    wait_bytes(WD.at[0, :, :, 0:2, 0, 0], s_loc.at[1])
    wait_bytes(WP.at[0:3, 0, 0, 0], s_loc.at[2])
    wait_bytes(WP.at[0:5, 0, 0, 0, 0], s_loc.at[3])

    pl.semaphore_wait(barrier, 127)

    def copy_to(ref, snd, rcv, to):
        return pltpu.make_async_remote_copy(
            src_ref=ref, dst_ref=ref, send_sem=snd, recv_sem=rcv, device_id=to, device_id_type=MESH
        )

    class Ring:
        def __init__(self, dim, sets, snd, rcv, sides, far):
            self.dim, self.sets, self.snd, self.rcv = dim, sets, snd, rcv
            self.sides, self.far = sides, far

        def at(self, step):
            return (pos[self.dim] + step + 4) % 4

        def send(self, ref, k, stage):
            copy_to(ref, self.snd, self.rcv.at[stage], near(self.dim, 1 if k == 0 else -1)).start()

        def start(self, hand):
            for part, half in self.sets:
                for k in range(2):
                    self.send(part(self.at(0)), k, 0)
            if hand:
                for part, half in self.sets:
                    hand(part(self.at(0)))

        def mid(self, hand):
            wait_bytes(self.sides, self.rcv.at[0])
            for part, half in self.sets:
                for k in range(2):
                    ref = half(self.at(-1 if k == 0 else 1), k)
                    if ref is not None:
                        self.send(ref, k, 1)
            if hand:
                for part, half in self.sets:
                    for k in (-1, 1):
                        hand(part(self.at(k)))

        def end(self, hand):
            wait_bytes(self.far, self.rcv.at[1])
            if hand:
                for part, half in self.sets:
                    hand(part(self.at(2)))

    hs = (slice(0, 2), slice(2, 4))

    def rings(b):
        def ring(n, dim, part, half, group, size):
            sets = [(functools.partial(part, W), functools.partial(half, W)) for W in (WS, WD)]
            spare = {1: (0, 0, 0), 4: (slice(None), 0, 0), 16: (slice(None), slice(None), 0)}[size]
            return Ring(
                dim, sets, w_snd.at[b, group], w_rcv.at[b, n],
                WD.at[(slice(0, 2), slice(0, 3)) + spare + (0,)], WD.at[(0, slice(0, 3)) + spare + (0,)],
            )

        def split(W, ref, h):
            if W is WS:
                return ref.at[pl.ds(16 * h, 16)]
            return ref if h == 0 else None

        return {
            "ay": ring(0, "y", lambda W, i: W.at[b, 0, :, i, z, c], lambda W, i, h: W.at[b, 0, hs[h], i, z, c], 1, 4),
            "by": ring(1, "y", lambda W, i: W.at[b, 1, x, i, z, c], lambda W, i, h: split(W, W.at[b, 1, x, i, z, c], h), 0, 1),
            "cz": ring(2, "z", lambda W, i: W.at[b, 2, x, y, i, c], lambda W, i, h: split(W, W.at[b, 2, x, y, i, c], h), 0, 1),
            "bz": ring(3, "z", lambda W, i: W.at[b, 1, x, :, i, c], lambda W, i, h: W.at[b, 1, x, hs[h], i, c], 1, 4),
            "cx": ring(4, "x", lambda W, i: W.at[b, 2, i, y, :, c], lambda W, i, h: W.at[b, 2, i, y, hs[h], c], 1, 4),
            "fz": ring(5, "z", lambda W, i: W.at[b, 0, :, :, i, c], lambda W, i, h: W.at[b, 0, hs[h], :, i, c], 2, 16),
            "fx": ring(6, "x", lambda W, i: W.at[b, 1, i, :, :, c], lambda W, i, h: W.at[b, 1, i, hs[h], :, c], 2, 16),
            "fy": ring(7, "y", lambda W, i: W.at[b, 2, :, i, :, c], lambda W, i, h: W.at[b, 2, hs[h], i, :, c], 2, 16),
        }

    def rings_p():
        def ring(n, dim, part, half, group, sides, far):
            return Ring(dim, [(part, half)], p_snd.at[group], p_rcv.at[n], sides, far)

        return {
            "ay": ring(0, "y", lambda i: WP.at[0:3, i, z, c], lambda i, h: WP.at[0:3, i, z, c, hs[h]], 0, WP.at[0:3, :, 0, :, 0], WP.at[0:3, :, 0, 0, 0]),
            "by": ring(1, "y", lambda i: WP.at[3:6, i, z, c, x], lambda i, h: WP.at[3 + h : 4 + 2 * h, i, z, c, x], 1, WP.at[0:6, 0, 0, 0, 0], WP.at[0:3, 0, 0, 0, 0]),
            "cz": ring(2, "z", lambda i: WP.at[6:8, y, i, c, x], lambda i, h: WP.at[6 + h : 7 + h, y, i, c, x], 1, WP.at[0:4, 0, 0, 0, 0], WP.at[0:2, 0, 0, 0, 0]),
            "bz": ring(3, "z", lambda i: WP.at[3:6, :, i, c, x], lambda i, h: WP.at[3:6, hs[h], i, c, x], 0, WP.at[0:3, :, 0, :, 0], WP.at[0:3, :, 0, 0, 0]),
            "cx": ring(4, "x", lambda i: WP.at[6:8, y, :, c, i], lambda i, h: WP.at[6:8, y, hs[h], c, i], 2, WP.at[0:4, :, 0, 0, 0], WP.at[0:2, :, 0, 0, 0]),
            "fz": ring(5, "z", lambda i: WP.at[0:3, :, i, c], lambda i, h: WP.at[0:3, hs[h], i, c], 3, WP.at[0:3, :, :, :, 0], WP.at[0:3, :, :, 0, 0]),
            "fx": ring(6, "x", lambda i: WP.at[3:6, :, :, c, i], lambda i, h: WP.at[3:6, hs[h], :, c, i], 3, WP.at[0:3, :, :, :, 0], WP.at[0:3, :, :, 0, 0]),
            "fy": ring(7, "y", lambda i: WP.at[6:8, i, :, c], lambda i, h: WP.at[6:8, i, hs[h], c], 4, WP.at[0:2, :, :, :, 0], WP.at[0:2, :, :, 0, 0]),
        }

    def over(k):
        def go(ref):
            copy_to(ref, d_snd.at[k], d_rcv.at[k], partner).start()

        return go

    def stage(n, b):
        if isinstance(b, int) and b == 4:
            r, give = rings_p(), over(4)
        else:
            r, give = rings(b), over(b)

        def each(names, what, hand=None):
            for name in names:
                what(r[name], hand)

        if n == 1:
            each(("by", "cz", "ay"), Ring.start)
        elif n == 2:
            each(("by", "cz", "ay"), Ring.mid)
        elif n == 3:
            each(("by", "cz"), Ring.end)
            each(("bz", "cx"), Ring.start)
        elif n == 4:
            each(("bz", "cx"), Ring.mid)
            each(("ay",), Ring.end)
        elif n == 5:
            each(("bz", "cx"), Ring.end)
            each(("fz", "fx", "fy"), Ring.start, give)
        elif n == 6:
            each(("fz", "fx", "fy"), Ring.mid, give)
        else:
            each(("fz", "fx", "fy"), Ring.end, give)

    def ready(b):
        wait_bytes(WD.at[0:3, :, :, :, :, 0], d_rcv.at[b])

    stage(1, 0)
    stage(1, 1)
    for to, n in peers(0, 1, 2, 3):
        pltpu.make_async_remote_copy(
            src_ref=send_z.at[n], dst_ref=recv_z.at[me],
            send_sem=s_snd.at[1], recv_sem=s_rcv.at[1], device_id=to, device_id_type=MESH,
        ).start()

    get_deter.wait()
    for k in range(8):
        lo = 512 * (k // 2) + 128 * (k % 2)
        parts = []
        for col in (lo, lo + 256):
            code = jnp.round(deter[:, col : col + 128] * SCALE)
            high = jnp.floor(code * (1.0 / 256.0))
            parts += [high.astype(BF), (code - high * 256.0).astype(BF)]
        got = dot(sel, jnp.concatenate(parts, axis=1))
        v0 = (got[:, 0:128] * 256.0 + got[:, 128:256]).astype(jnp.int32)
        v1 = (got[:, 256:384] * 256.0 + got[:, 384:512]).astype(jnp.int32)
        word = v1 * 65536 + (v0 + 32768)
        send[pl.ds(k, 128, stride=16), :] = word[0:128]
        send[pl.ds(8 + k, 128, stride=16), :] = word[128:256]
        if k == 2:
            stage(2, 0)

    def rows_of(n):
        return pl.ds(pl.multiple_of(n * 16, 16), 16)

    def send_rows(group):
        for to, n in peers(group):
            pltpu.make_async_remote_copy(
                src_ref=send.at[rows_of(n), :], dst_ref=recv.at[rows_of(me), :],
                send_sem=s_snd.at[0], recv_sem=s_rcv.at[0], device_id=to, device_id_type=MESH,
            ).start()

    stage(3, 0)
    send_rows(0)
    stage(2, 1)
    stage(1, 2)
    own = [
        pltpu.make_async_copy(send.at[rows_of(me), :], recv.at[rows_of(me), :], s_loc.at[4]),
        pltpu.make_async_copy(send_z.at[me], recv_z.at[me], s_loc.at[5]),
    ]
    for cp in own:
        cp.start()

    E = spread(32, 1024)
    cls = (lax.broadcasted_iota(jnp.int32, (256, 1024), 1) % 32).astype(F32)

    def one_hot(t):
        rep = dot(samps_t[t - 1].astype(F32).astype(BF), E, ((0,), (0,)))
        OH[256 * t : 256 * t + 256, :] = jnp.where(rep == cls, 1.0, 0.0).astype(BF)

    def act_terms(b):
        def piece(n, u):
            p, e = n // 2, n % 2
            cols = pl.ds(pl.multiple_of(b * 1536 + n * 256, 256), 256)
            PRE[b, p, :, pl.ds(pl.multiple_of(e * 256, 256), 256)] = dot(AH[...], ACT[:, cols])
            return u

        lax.fori_loop(0, 6, piece, 0)

    one_hot(1)
    one_hot(2)
    stage(4, 0)
    stage(3, 1)
    send_rows(1)
    stage(2, 2)
    one_hot(3)
    ACT[...] = jnp.zeros_like(ACT)
    ACT[0 : act.shape[0], :] = act[...]
    which = lax.broadcasted_iota(jnp.int32, (32, 256), 0)
    for t in range(STEPS):
        a_hot = jnp.where(which == acts_t[t : t + 1, :], 1.0, 0.0)
        AH[256 * t : 256 * t + 256, :] = jnp.transpose(a_hot).astype(BF)
    stage(5, 0)
    stage(1, 3)
    act_terms(0)
    stage(4, 1)
    stage(3, 2)
    send_rows(2)
    act_terms(1)
    act_terms(2)
    act_terms(3)
    stage(6, 0)
    stage(5, 1)
    send_rows(3)
    stage(2, 3)

    wait_bytes(recv_z.at[pl.ds(0, 127)], s_rcv.at[1])
    own[1].wait()
    zv = recv_z[...].reshape(128, 128)
    zf[pl.ds(0, 128, stride=2), :] = zv
    zf[pl.ds(1, 128, stride=2), :] = pltpu.roll(zv, 96, 1)
    codes = zf[...].astype(F32)
    rep = dot(codes[:, 0:32].astype(BF), E)
    OH[0:256, :] = jnp.where(rep == cls, 1.0, 0.0).astype(BF)
    alive = jnp.where(codes < 32.0, 1.0, 0.0)
    lane0 = jnp.where(lax.broadcasted_iota(jnp.int32, (8, 128), 1) == 0, 1.0, 0.0).astype(BF)
    live_out[...] = dot(lane0, alive.astype(BF), ((1,), (1,)))
    live_col = alive[:, 0:1]
    stage(7, 0)
    ready(0)

    def start_rows():
        wait_bytes(recv.at[pl.ds(0, 127 * 16), :], s_rcv.at[0])
        own[0].wait()
        for k in range(8):
            word = recv[pl.ds(k, 256, stride=8), :]
            v1 = lax.shift_right_arithmetic(word, 16)
            v0 = (word & 65535) - 32768
            b, e = k // 2, (k % 2) * 128
            H0[b, :, e : e + 128] = v0.astype(F32) * (1.0 / SCALE)
            H0[b, :, 256 + e : 384 + e] = v1.astype(F32) * (1.0 / SCALE)

    def put_prior(e, k):
        return pltpu.make_async_copy(WP.at[:, :, :, e], wp_out.at[:, :, :, e], s_out.at[k])

    def put_states(b):
        return pltpu.make_async_copy(ST.at[b % 2], st_out.at[b], s_out.at[b])

    def compute(b, u):
        def gate(p):
            def piece(e, u):
                rhs = jnp.concatenate(
                    [WS[b, p, 2 * e + i].reshape(1024, 128) for i in range(2)], axis=1
                )
                cols = pl.ds(pl.multiple_of(e * 256, 256), 256)
                PRE[b, p, :, cols] = PRE[b, p, :, cols] + dot(OH[...], rhs)
                return u

            lax.fori_loop(0, 2, piece, 0)

        def also(plan):
            for when, stages in plan.items():

                @pl.when(b == when)
                def _():
                    for n, k in stages:
                        stage(n, k)

        gate(0)
        also({0: ((4, 2), (1, 4)), 1: ((6, 2), (3, 4)), 2: ((6, 3),), 3: ((6, 4),)})
        gate(1)
        also({0: ((6, 1), (3, 3)), 1: ((5, 3),), 2: ((5, 4),)})
        gate(2)

        @pl.when(b == 0)
        def _():
            stage(5, 2)
            start_rows()

        H[...] = H0[b]

        @pl.when(b >= 2)
        def _():
            put_states(b - 2).wait()

        def step(t, u):
            h = H[...]
            low = h.astype(BF)
            rows = pl.ds(pl.multiple_of(t * 256, 256), 256)

            def gates(p):
                rhs = jnp.concatenate([WD[b, p, q].reshape(512, 128) for q in range(4)], axis=1)
                return PRE[b, p, rows, :] + dot(low, rhs)

            cand = jnp.tanh(sig(gates(0)) * gates(1))
            g = sig(gates(2) - 1.0)
            new = g * cand + (1.0 - g) * h
            H[...] = new
            ST[b % 2, t] = (new * live_col).astype(BF)
            return u

        lax.fori_loop(0, 2, step, 0)

        @pl.when(b < 3)
        def _():
            stage(7, b + 1)

        also({0: ((2, 4),), 3: ((7, 4),)})

        @pl.when(b == 3)
        def _():
            put_prior(c, 4).start()

        lax.fori_loop(2, STEPS, step, 0)
        put_states(b).start()

        also({0: ((4, 3),), 1: ((4, 4),)})

        @pl.when(b < 3)
        def _():
            ready(b + 1)

        return u

    lax.fori_loop(0, BLOCKS, compute, 0)
    wait_bytes(WP.at[:, :, :, 0], d_rcv.at[4])
    put_prior(1 - c, 5).start()
    wait_bytes(send.at[pl.ds(0, 127 * 16), :], s_snd.at[0])
    wait_bytes(send_z.at[pl.ds(0, 127)], s_snd.at[1])

    def drain(b, u):
        wait_bytes(WD.at[0, :, 0:3, 0:2, 0, 0], w_snd.at[b, 0])
        wait_bytes(WD.at[0, :, 0:3, 0:3, :, 0], w_snd.at[b, 1])
        wait_bytes(WD.at[0:2, :, 0:3, :, 0:3, :], w_snd.at[b, 2])
        wait_bytes(WD.at[0:3, :, :, :, :, 0], d_snd.at[b])

        @pl.when(b >= 2)
        def _():
            put_states(b).wait()

        return u

    lax.fori_loop(0, BLOCKS, drain, 0)
    wait_bytes(WP.at[0:3, :, 0:3, :, 0], p_snd.at[0])
    wait_bytes(WP.at[0:5, 0:3, 0, 0, 0], p_snd.at[1])
    wait_bytes(WP.at[0:3, :, 0, :, 0], p_snd.at[2])
    wait_bytes(WP.at[0:3, :, :, :, 0:3], p_snd.at[3])
    wait_bytes(WP.at[0:3, :, :, :, 0], p_snd.at[4])
    wait_bytes(WP.at[:, :, :, 0], d_snd.at[4])
    put_prior(c, 4).wait()
    put_prior(1 - c, 5).wait()


def prior_kernel(st, wp, live, samps_t, img, lp, stv, wpv, hot, scr, imgv, la, lb, s_in, s_w, s_out):
    def part(s):
        return pl.ds(pl.multiple_of(s * 128, 128), 128)

    def get_w(n):
        return pltpu.make_async_copy(wp.at[pl.ds(2 * n, 2)], wpv.at[pl.ds(2 * n, 2)], s_w.at[n])

    def get_s(s):
        return pltpu.make_async_copy(st.at[:, :, part(s)], stv.at[:, :, part(s)], s_in.at[s])

    def put(s):
        return pltpu.make_async_copy(imgv.at[part(s)], img.at[part(s)], s_out.at[s])

    get_s(0).start()
    get_w(0).start()
    get_w(1).start()
    get_s(1).start()
    get_w(2).start()
    get_w(3).start()
    E = spread(32, 1024)
    E8 = spread(8, 256)
    cls = (lax.broadcasted_iota(jnp.int32, (256, 1024), 1) % 32).astype(F32)
    lb[...] = jnp.zeros_like(lb)

    def hits(t, u):
        rep = dot(samps_t[t].astype(F32).astype(BF), E, ((0,), (0,)))
        hot[t] = jnp.where(rep == cls, 1.0, 0.0).astype(BF)
        return u

    lax.fori_loop(0, STEPS, hits, 0)

    def product(s, n):
        low = jnp.concatenate([stv[b, :, part(s)].reshape(512, 512) for b in range(BLOCKS)], axis=1)
        rhs = jnp.concatenate([wpv[2 * n + i].reshape(2048, 128) for i in range(2)], axis=1)
        return dot(low, rhs)

    def scores(logits, s, n):
        def grouped(v):
            hi = v.astype(BF)
            low = (v - hi.astype(F32)).astype(BF)
            return dot(E8, hi, ((1,), (1,))) + dot(E8, low, ((1,), (1,)))

        cols = pl.ds(pl.multiple_of(n * 256, 256), 256)
        total = jnp.log(grouped(jnp.exp(logits)))
        hit = grouped(logits * hot[:, part(s), cols].reshape(512, 256).astype(F32))
        value = hit - total
        for t in range(STEPS):
            lp[t, pl.ds(pl.multiple_of(n * 8, 8), 8), part(s)] = jnp.where(
                live[:, part(s)] > 0.0, value[:, 128 * t : 128 * t + 128], 0.0
            )

    def trip(j, u):
        @pl.when(j < 2)
        def _():
            get_s(j).wait()

            def lay(b, u):
                for t in range(STEPS):
                    scr[:, t, :] = stv[b, t, part(j)].astype(F32)
                cols = pl.ds(pl.multiple_of(b * 512, 512), 512)
                imgv[part(j), :, cols] = scr[...].astype(BF)
                return u

            lax.fori_loop(0, BLOCKS, lay, 0)
            put(j).start()
            get_w(2 * j).wait()
            get_w(2 * j + 1).wait()

        s, n = j // 2, 2 * (j % 2)
        last = (2 * j + 7) % 8
        la[...] = product(s, n)
        scores(lb[...], last // 4, last % 4)
        lb[...] = product(s, n + 1)
        scores(la[...], s, n)
        return u

    lax.fori_loop(0, 4, trip, 0)
    scores(lb[...], 1, 3)
    put(0).wait()
    put(1).wait()


def on_device(deter, stoch, rows, counts, acts, samps, w_s, w_d, act, w_p):
    vmem = pl.BlockSpec(memory_space=pltpu.VMEM)
    hbm = pl.BlockSpec(memory_space=pl.ANY)
    dma = pltpu.SemaphoreType.DMA
    samps_t = samps.transpose(1, 2, 0)
    states, wp, live = pl.pallas_call(
        gru_kernel,
        name="gru",
        out_shape=(
            jax.ShapeDtypeStruct((4, 4, 256, 512), BF),
            jax.ShapeDtypeStruct((8, 4, 4, 2, 4, 16, 128), BF),
            jax.ShapeDtypeStruct((8, 256), F32),
        ),
        in_specs=[hbm] + [vmem] * 5 + [hbm, hbm, vmem, hbm],
        out_specs=(hbm, hbm, vmem),
        scratch_shapes=[
            pltpu.VMEM((256, 2048), F32),
            pltpu.VMEM((4, 3, 4, 4, 4, 2, 32, 128), BF),
            pltpu.VMEM((4, 3, 4, 4, 4, 2, 16, 128), BF),
            pltpu.VMEM((8, 4, 4, 2, 4, 16, 128), BF),
            pltpu.VMEM((2048, 128), jnp.int32),
            pltpu.VMEM((2048, 128), jnp.int32),
            pltpu.VMEM((128, 1, 128), jnp.int32),
            pltpu.VMEM((128, 1, 128), jnp.int32),
            pltpu.VMEM((256, 128), jnp.int32),
            pltpu.VMEM((4, 256, 512), F32),
            pltpu.VMEM((256, 512), F32),
            pltpu.VMEM((1024, 1024), BF),
            pltpu.VMEM((32, 6144), BF),
            pltpu.VMEM((1024, 32), BF),
            pltpu.VMEM((4, 3, 1024, 512), F32),
            pltpu.VMEM((2, 4, 256, 512), BF),
            dma((7,)), dma((2,)), dma((2,)),
            dma((4, 3)), dma((4, 8, 2)),
            dma((5,)), dma((8, 2)),
            dma((5,)), dma((5,)), dma((6,)),
        ],
        compiler_params=pltpu.CompilerParams(
            collective_id=0, has_side_effects=True, vmem_limit_bytes=63 * 1024 * 1024
        ),
    )(deter, stoch.T, rows.T, counts, acts.T, samps_t, w_s, w_d, act, w_p)
    imagined, logp = pl.pallas_call(
        prior_kernel,
        name="prior",
        out_shape=(
            jax.ShapeDtypeStruct((256, 4, 2048), BF),
            jax.ShapeDtypeStruct((4, 32, 256), F32),
        ),
        in_specs=[hbm, hbm, vmem, vmem],
        out_specs=(hbm, vmem),
        scratch_shapes=[
            pltpu.VMEM((4, 4, 256, 512), BF),
            pltpu.VMEM((8, 4, 4, 2, 4, 16, 128), BF),
            pltpu.VMEM((4, 256, 1024), BF),
            pltpu.VMEM((128, 4, 512), F32),
            pltpu.VMEM((256, 4, 2048), BF),
            pltpu.VMEM((512, 256), F32),
            pltpu.VMEM((512, 256), F32),
            dma((2,)), dma((4,)), dma((2,)),
        ],
        compiler_params=pltpu.CompilerParams(vmem_limit_bytes=60 * 1024 * 1024),
    )(states, wp, live, samps_t)
    return (imagined, logp.transpose(2, 0, 1))


def solution(mesh):
    in_specs = (
        P(("gx", "gy"), None),
        P(("gx", "gy"), None),
        P(("gx", "gy"), None),
        P(("gx", "gy"), None),
        P(("gx", "gy"), None),
        P(("gx", "gy"), None, None),
        P("gy", None),
        P(None, "gy", None),
        P(),
        P("gy", None),
    )
    out_specs = (P(("gx", "gy"), None, None), P(("gx", "gy"), None, None))
    return jax.shard_map(
        on_device, mesh=mesh, in_specs=in_specs, out_specs=out_specs, check_vma=False
    )
```

```python
import functools

import jax
import jax.numpy as jnp
from jax import lax
from jax.experimental import pallas as pl
from jax.experimental.pallas import tpu as pltpu
from jax.sharding import PartitionSpec as P

STEPS = 4
BLOCKS = 4
BF = jnp.bfloat16
F32 = jnp.float32
MESH = pl.DeviceIdType.MESH
SCALE = 32767.0


def dot(a, b, dims=((1,), (0,))):
    return lax.dot_general(a, b, (dims, ((), ())), preferred_element_type=F32)


def spread(rows, lanes):
    g = lax.broadcasted_iota(jnp.int32, (rows, lanes), 0)
    k = lax.broadcasted_iota(jnp.int32, (rows, lanes), 1)
    return jnp.where((k >= g * 32) & (k < g * 32 + 32), 1.0, 0.0).astype(BF)


def sig(v):
    return 0.5 * jnp.tanh(0.5 * v) + 0.5


def gru_kernel(
    deter_h, stoch_t, rows_t, counts, acts_t, samps_t, w_s, w_d, act, w_p,
    st_out, wp_out, live_out,
    deter, WS, WD, WP, send, recv, send_z, recv_z, zf, H0, H, OH, ACT, AH, PRE, ST,
    s_loc, s_snd, s_rcv, w_snd, w_rcv, p_snd, p_rcv, d_snd, d_rcv, s_out,
):
    x = lax.axis_index("gx")
    gy = lax.axis_index("gy")
    y, z, c = gy // 8, (gy // 2) % 4, gy % 2
    me = x * 32 + gy

    def dev(tx, ty, tz, tc):
        return (tx, ty * 8 + tz * 2 + tc)

    def near(dim, step):
        s = (step + 4) % 4
        if dim == "x":
            return dev((x + s) % 4, y, z, c)
        if dim == "y":
            return dev(x, (y + s) % 4, z, c)
        return dev(x, y, (z + s) % 4, c)

    pos = {"x": x, "y": y, "z": z}
    partner = dev(x, y, z, 1 - c)

    def wait_bytes(ref, sem):
        pltpu.make_async_copy(ref, ref, sem).wait()

    barrier = pltpu.get_barrier_semaphore()

    xs, ys, zs = ([(v + i) % 4 for i in range(4)] for v in (x, y, z))
    y8, z2, cs = [v * 8 for v in ys], [v * 2 for v in zs], [c, 1 - c]

    def peers(*groups):
        for dx in range(4):
            for dy in range(4):
                for dz in range(4):
                    for dc in range(2):
                        if dx + dy + dz + dc > 0 and (dx + dy + dz) % 4 in groups:
                            g = y8[dy] + (z2[dz] + cs[dc])
                            yield (xs[dx], g), xs[dx] * 32 + g

    for to, _ in reversed(list(peers(0, 1, 2, 3))):
        pl.semaphore_signal(barrier, inc=1, device_id=to, device_id_type=MESH)
    get_deter = pltpu.make_async_copy(deter_h, deter, s_loc.at[6])

    def fill(b, u):
        for p in range(3):
            for q in range(4) if p == 0 else (x,):
                col = pl.multiple_of(b * 1536 + p * 512 + q * 128, 128)
                pltpu.make_async_copy(
                    w_s.at[:, pl.ds(col, 128)], WS.at[b, p, q, y, z, c], s_loc.at[0]
                ).start()
                col = pl.multiple_of(p * 512 + q * 128, 128)
                pltpu.make_async_copy(
                    w_d.at[b, :, pl.ds(col, 128)], WD.at[b, p, q, y, z, c], s_loc.at[1]
                ).start()
        return u

    lax.fori_loop(0, 4, fill, 0)
    for j in range(8):
        if j < 3:
            for q in range(4):
                pltpu.make_async_copy(
                    w_p.at[pl.ds(q * 16, 16), pl.ds(j * 128, 128)], WP.at[j, y, z, c, q], s_loc.at[2]
                ).start()
        else:
            pltpu.make_async_copy(
                w_p.at[pl.ds(pl.multiple_of(x * 16, 16), 16), pl.ds(j * 128, 128)],
                WP.at[j, y, z, c, x],
                s_loc.at[3],
            ).start()
    get_deter.start()

    iota = lax.broadcasted_iota(jnp.int32, (256, 128), 0)
    sel_t = jnp.concatenate(
        [jnp.where(iota == rows_t[i : i + 1, :], 1.0, 0.0) for i in range(2)], axis=1
    )
    sel = jnp.transpose(sel_t).astype(BF)
    picked = dot(stoch_t[...].astype(F32).astype(BF), sel_t.astype(BF))
    zv = [
        jnp.where(counts[...] > i, picked[:, 128 * i : 128 * i + 128], 64.0) for i in range(2)
    ]
    zv = jnp.concatenate(zv + [jnp.zeros((64, 128), F32)], axis=0)
    send_z[...] = jnp.transpose(zv).astype(jnp.int32).reshape(128, 1, 128)

    wait_bytes(WS.at[0, :, :, 0:2, 0, 0], s_loc.at[0])
    wait_bytes(WD.at[0, :, :, 0:2, 0, 0], s_loc.at[1])
    wait_bytes(WP.at[0:3, 0, 0, 0], s_loc.at[2])
    wait_bytes(WP.at[0:5, 0, 0, 0, 0], s_loc.at[3])

    pl.semaphore_wait(barrier, 127)

    def copy_to(ref, snd, rcv, to):
        return pltpu.make_async_remote_copy(
            src_ref=ref, dst_ref=ref, send_sem=snd, recv_sem=rcv, device_id=to, device_id_type=MESH
        )

    class Ring:
        def __init__(self, dim, sets, snd, rcv, sides, far):
            self.dim, self.sets, self.snd, self.rcv = dim, sets, snd, rcv
            self.sides, self.far = sides, far

        def at(self, step):
            return (pos[self.dim] + step + 4) % 4

        def send(self, ref, k, stage):
            copy_to(ref, self.snd, self.rcv.at[stage], near(self.dim, 1 if k == 0 else -1)).start()

        def start(self, hand):
            for part, half in self.sets:
                for k in range(2):
                    self.send(part(self.at(0)), k, 0)
            if hand:
                for part, half in self.sets:
                    hand(part(self.at(0)))

        def mid(self, hand):
            wait_bytes(self.sides, self.rcv.at[0])
            for part, half in self.sets:
                for k in range(2):
                    ref = half(self.at(-1 if k == 0 else 1), k)
                    if ref is not None:
                        self.send(ref, k, 1)
            if hand:
                for part, half in self.sets:
                    for k in (-1, 1):
                        hand(part(self.at(k)))

        def end(self, hand):
            wait_bytes(self.far, self.rcv.at[1])
            if hand:
                for part, half in self.sets:
                    hand(part(self.at(2)))

    hs = (slice(0, 2), slice(2, 4))

    def rings(b):
        def ring(n, dim, part, half, group, size):
            sets = [(functools.partial(part, W), functools.partial(half, W)) for W in (WS, WD)]
            spare = {1: (0, 0, 0), 4: (slice(None), 0, 0), 16: (slice(None), slice(None), 0)}[size]
            return Ring(
                dim, sets, w_snd.at[b, group], w_rcv.at[b, n],
                WD.at[(slice(0, 2), slice(0, 3)) + spare + (0,)], WD.at[(0, slice(0, 3)) + spare + (0,)],
            )

        def split(W, ref, h):
            if W is WS:
                return ref.at[pl.ds(16 * h, 16)]
            return ref if h == 0 else None

        return {
            "ay": ring(0, "y", lambda W, i: W.at[b, 0, :, i, z, c], lambda W, i, h: W.at[b, 0, hs[h], i, z, c], 1, 4),
            "by": ring(1, "y", lambda W, i: W.at[b, 1, x, i, z, c], lambda W, i, h: split(W, W.at[b, 1, x, i, z, c], h), 0, 1),
            "cz": ring(2, "z", lambda W, i: W.at[b, 2, x, y, i, c], lambda W, i, h: split(W, W.at[b, 2, x, y, i, c], h), 0, 1),
            "bz": ring(3, "z", lambda W, i: W.at[b, 1, x, :, i, c], lambda W, i, h: W.at[b, 1, x, hs[h], i, c], 1, 4),
            "cx": ring(4, "x", lambda W, i: W.at[b, 2, i, y, :, c], lambda W, i, h: W.at[b, 2, i, y, hs[h], c], 1, 4),
            "fz": ring(5, "z", lambda W, i: W.at[b, 0, :, :, i, c], lambda W, i, h: W.at[b, 0, hs[h], :, i, c], 2, 16),
            "fx": ring(6, "x", lambda W, i: W.at[b, 1, i, :, :, c], lambda W, i, h: W.at[b, 1, i, hs[h], :, c], 2, 16),
            "fy": ring(7, "y", lambda W, i: W.at[b, 2, :, i, :, c], lambda W, i, h: W.at[b, 2, hs[h], i, :, c], 2, 16),
        }

    def rings_p():
        def ring(n, dim, part, half, group, sides, far):
            return Ring(dim, [(part, half)], p_snd.at[group], p_rcv.at[n], sides, far)

        return {
            "ay": ring(0, "y", lambda i: WP.at[0:3, i, z, c], lambda i, h: WP.at[0:3, i, z, c, hs[h]], 0, WP.at[0:3, :, 0, :, 0], WP.at[0:3, :, 0, 0, 0]),
            "by": ring(1, "y", lambda i: WP.at[3:6, i, z, c, x], lambda i, h: WP.at[3 + h : 4 + 2 * h, i, z, c, x], 1, WP.at[0:6, 0, 0, 0, 0], WP.at[0:3, 0, 0, 0, 0]),
            "cz": ring(2, "z", lambda i: WP.at[6:8, y, i, c, x], lambda i, h: WP.at[6 + h : 7 + h, y, i, c, x], 1, WP.at[0:4, 0, 0, 0, 0], WP.at[0:2, 0, 0, 0, 0]),
            "bz": ring(3, "z", lambda i: WP.at[3:6, :, i, c, x], lambda i, h: WP.at[3:6, hs[h], i, c, x], 0, WP.at[0:3, :, 0, :, 0], WP.at[0:3, :, 0, 0, 0]),
            "cx": ring(4, "x", lambda i: WP.at[6:8, y, :, c, i], lambda i, h: WP.at[6:8, y, hs[h], c, i], 2, WP.at[0:4, :, 0, 0, 0], WP.at[0:2, :, 0, 0, 0]),
            "fz": ring(5, "z", lambda i: WP.at[0:3, :, i, c], lambda i, h: WP.at[0:3, hs[h], i, c], 3, WP.at[0:3, :, :, :, 0], WP.at[0:3, :, :, 0, 0]),
            "fx": ring(6, "x", lambda i: WP.at[3:6, :, :, c, i], lambda i, h: WP.at[3:6, hs[h], :, c, i], 3, WP.at[0:3, :, :, :, 0], WP.at[0:3, :, :, 0, 0]),
            "fy": ring(7, "y", lambda i: WP.at[6:8, i, :, c], lambda i, h: WP.at[6:8, i, hs[h], c], 4, WP.at[0:2, :, :, :, 0], WP.at[0:2, :, :, 0, 0]),
        }

    def over(k):
        def go(ref):
            copy_to(ref, d_snd.at[k], d_rcv.at[k], partner).start()

        return go

    def stage(n, b):
        if isinstance(b, int) and b == 4:
            r, give = rings_p(), over(4)
        else:
            r, give = rings(b), over(b)

        def each(names, what, hand=None):
            for name in names:
                what(r[name], hand)

        if n == 1:
            each(("by", "cz", "ay"), Ring.start)
        elif n == 2:
            each(("by", "cz", "ay"), Ring.mid)
        elif n == 3:
            each(("by", "cz"), Ring.end)
            each(("bz", "cx"), Ring.start)
        elif n == 4:
            each(("bz", "cx"), Ring.mid)
            each(("ay",), Ring.end)
        elif n == 5:
            each(("bz", "cx"), Ring.end)
            each(("fz", "fx", "fy"), Ring.start, give)
        elif n == 6:
            each(("fz", "fx", "fy"), Ring.mid, give)
        else:
            each(("fz", "fx", "fy"), Ring.end, give)

    def ready(b):
        wait_bytes(WD.at[0:3, :, :, :, :, 0], d_rcv.at[b])

    stage(1, 0)
    stage(1, 1)
    for to, n in peers(0, 1, 2, 3):
        pltpu.make_async_remote_copy(
            src_ref=send_z.at[n], dst_ref=recv_z.at[me],
            send_sem=s_snd.at[1], recv_sem=s_rcv.at[1], device_id=to, device_id_type=MESH,
        ).start()

    get_deter.wait()
    for k in range(8):
        lo = 512 * (k // 2) + 128 * (k % 2)
        parts = []
        for col in (lo, lo + 256):
            code = jnp.round(deter[:, col : col + 128] * SCALE)
            high = jnp.floor(code * (1.0 / 256.0))
            parts += [high.astype(BF), (code - high * 256.0).astype(BF)]
        got = dot(sel, jnp.concatenate(parts, axis=1))
        v0 = (got[:, 0:128] * 256.0 + got[:, 128:256]).astype(jnp.int32)
        v1 = (got[:, 256:384] * 256.0 + got[:, 384:512]).astype(jnp.int32)
        word = v1 * 65536 + (v0 + 32768)
        send[pl.ds(k, 128, stride=16), :] = word[0:128]
        send[pl.ds(8 + k, 128, stride=16), :] = word[128:256]
        if k == 2:
            stage(2, 0)

    def rows_of(n):
        return pl.ds(pl.multiple_of(n * 16, 16), 16)

    def send_rows(group):
        for to, n in peers(group):
            pltpu.make_async_remote_copy(
                src_ref=send.at[rows_of(n), :], dst_ref=recv.at[rows_of(me), :],
                send_sem=s_snd.at[0], recv_sem=s_rcv.at[0], device_id=to, device_id_type=MESH,
            ).start()

    stage(3, 0)
    send_rows(0)
    stage(2, 1)
    stage(1, 2)
    own = [
        pltpu.make_async_copy(send.at[rows_of(me), :], recv.at[rows_of(me), :], s_loc.at[4]),
        pltpu.make_async_copy(send_z.at[me], recv_z.at[me], s_loc.at[5]),
    ]
    for cp in own:
        cp.start()

    E = spread(32, 1024)
    cls = (lax.broadcasted_iota(jnp.int32, (256, 1024), 1) % 32).astype(F32)

    def one_hot(t):
        rep = dot(samps_t[t - 1].astype(F32).astype(BF), E, ((0,), (0,)))
        OH[256 * t : 256 * t + 256, :] = jnp.where(rep == cls, 1.0, 0.0).astype(BF)

    def act_terms(b):
        def piece(n, u):
            p, e = n // 2, n % 2
            cols = pl.ds(pl.multiple_of(b * 1536 + n * 256, 256), 256)
            PRE[b, p, :, pl.ds(pl.multiple_of(e * 256, 256), 256)] = dot(AH[...], ACT[:, cols])
            return u

        lax.fori_loop(0, 6, piece, 0)

    one_hot(1)
    one_hot(2)
    stage(4, 0)
    stage(3, 1)
    send_rows(1)
    stage(2, 2)
    one_hot(3)
    ACT[...] = jnp.zeros_like(ACT)
    ACT[0 : act.shape[0], :] = act[...]
    which = lax.broadcasted_iota(jnp.int32, (32, 256), 0)
    for t in range(STEPS):
        a_hot = jnp.where(which == acts_t[t : t + 1, :], 1.0, 0.0)
        AH[256 * t : 256 * t + 256, :] = jnp.transpose(a_hot).astype(BF)
    stage(5, 0)
    stage(1, 3)
    act_terms(0)
    stage(4, 1)
    stage(3, 2)
    act_terms(1)
    act_terms(2)
    stage(6, 0)
    send_rows(2)
    act_terms(3)
    stage(5, 1)
    send_rows(3)
    stage(2, 3)

    wait_bytes(recv_z.at[pl.ds(0, 127)], s_rcv.at[1])
    own[1].wait()
    zv = recv_z[...].reshape(128, 128)
    zf[pl.ds(0, 128, stride=2), :] = zv
    zf[pl.ds(1, 128, stride=2), :] = pltpu.roll(zv, 96, 1)
    codes = zf[...].astype(F32)
    rep = dot(codes[:, 0:32].astype(BF), E)
    OH[0:256, :] = jnp.where(rep == cls, 1.0, 0.0).astype(BF)
    alive = jnp.where(codes < 32.0, 1.0, 0.0)
    lane0 = jnp.where(lax.broadcasted_iota(jnp.int32, (8, 128), 1) == 0, 1.0, 0.0).astype(BF)
    live_out[...] = dot(lane0, alive.astype(BF), ((1,), (1,)))
    live_col = alive[:, 0:1]
    stage(7, 0)
    ready(0)

    def start_rows():
        wait_bytes(recv.at[pl.ds(0, 127 * 16), :], s_rcv.at[0])
        own[0].wait()
        for k in range(8):
            word = recv[pl.ds(k, 256, stride=8), :]
            v1 = lax.shift_right_arithmetic(word, 16)
            v0 = (word & 65535) - 32768
            b, e = k // 2, (k % 2) * 128
            H0[b, :, e : e + 128] = v0.astype(F32) * (1.0 / SCALE)
            H0[b, :, 256 + e : 384 + e] = v1.astype(F32) * (1.0 / SCALE)

    def put_prior(e, k):
        return pltpu.make_async_copy(WP.at[:, :, :, e], wp_out.at[:, :, :, e], s_out.at[k])

    def put_states(b):
        return pltpu.make_async_copy(ST.at[b % 2], st_out.at[b], s_out.at[b])

    def compute(b, u):
        def gate(p):
            def piece(e, u):
                rhs = jnp.concatenate(
                    [WS[b, p, 2 * e + i].reshape(1024, 128) for i in range(2)], axis=1
                )
                cols = pl.ds(pl.multiple_of(e * 256, 256), 256)
                PRE[b, p, :, cols] = PRE[b, p, :, cols] + dot(OH[...], rhs)
                return u

            lax.fori_loop(0, 2, piece, 0)

        def also(plan):
            for when, stages in plan.items():

                @pl.when(b == when)
                def _():
                    for n, k in stages:
                        stage(n, k)

        gate(0)
        also({0: ((4, 2), (1, 4)), 1: ((6, 2), (3, 4)), 2: ((6, 3),), 3: ((6, 4),)})
        gate(1)
        also({0: ((6, 1), (3, 3)), 1: ((5, 3),), 2: ((5, 4),)})
        gate(2)

        @pl.when(b == 0)
        def _():
            stage(5, 2)
            start_rows()

        H[...] = H0[b]

        @pl.when(b >= 2)
        def _():
            put_states(b - 2).wait()

        def step(t, u):
            h = H[...]
            low = h.astype(BF)
            rows = pl.ds(pl.multiple_of(t * 256, 256), 256)

            for e in range(2):
                cols = slice(256 * e, 256 * e + 256)

                def gates(p):
                    rhs = [WD[b, p, q].reshape(512, 128) for q in range(2 * e, 2 * e + 2)]
                    return PRE[b, p, rows, cols] + dot(low, jnp.concatenate(rhs, axis=1))

                cand = jnp.tanh(sig(gates(0)) * gates(1))
                g = sig(gates(2) - 1.0)
                new = g * cand + (1.0 - g) * h[:, cols]
                H[:, cols] = new
                ST[b % 2, t, :, cols] = (new * live_col).astype(BF)
            return u

        lax.fori_loop(0, 2, step, 0)

        @pl.when(b < 3)
        def _():
            stage(7, b + 1)

        also({0: ((2, 4),), 3: ((7, 4),)})

        @pl.when(b == 3)
        def _():
            put_prior(c, 4).start()

        lax.fori_loop(2, STEPS, step, 0)
        put_states(b).start()

        also({0: ((4, 3),), 1: ((4, 4),)})

        @pl.when(b < 3)
        def _():
            ready(b + 1)

        return u

    lax.fori_loop(0, BLOCKS, compute, 0)
    wait_bytes(WP.at[:, :, :, 0], d_rcv.at[4])
    put_prior(1 - c, 5).start()
    wait_bytes(send.at[pl.ds(0, 127 * 16), :], s_snd.at[0])
    wait_bytes(send_z.at[pl.ds(0, 127)], s_snd.at[1])

    def drain(b, u):
        wait_bytes(WD.at[0, :, 0:3, 0:2, 0, 0], w_snd.at[b, 0])
        wait_bytes(WD.at[0, :, 0:3, 0:3, :, 0], w_snd.at[b, 1])
        wait_bytes(WD.at[0:2, :, 0:3, :, 0:3, :], w_snd.at[b, 2])
        wait_bytes(WD.at[0:3, :, :, :, :, 0], d_snd.at[b])

        @pl.when(b >= 2)
        def _():
            put_states(b).wait()

        return u

    lax.fori_loop(0, BLOCKS, drain, 0)
    wait_bytes(WP.at[0:3, :, 0:3, :, 0], p_snd.at[0])
    wait_bytes(WP.at[0:5, 0:3, 0, 0, 0], p_snd.at[1])
    wait_bytes(WP.at[0:3, :, 0, :, 0], p_snd.at[2])
    wait_bytes(WP.at[0:3, :, :, :, 0:3], p_snd.at[3])
    wait_bytes(WP.at[0:3, :, :, :, 0], p_snd.at[4])
    wait_bytes(WP.at[:, :, :, 0], d_snd.at[4])
    put_prior(c, 4).wait()
    put_prior(1 - c, 5).wait()


def prior_kernel(st, wp, live, samps_t, img, lp, stv, wpv, hot, scr, imgv, la, lb, s_in, s_w, s_out):
    def part(s):
        return pl.ds(pl.multiple_of(s * 128, 128), 128)

    def get_w(n):
        return pltpu.make_async_copy(wp.at[pl.ds(2 * n, 2)], wpv.at[pl.ds(2 * n, 2)], s_w.at[n])

    def get_s(s):
        return pltpu.make_async_copy(st.at[:, :, part(s)], stv.at[:, :, part(s)], s_in.at[s])

    def put(s):
        return pltpu.make_async_copy(imgv.at[part(s)], img.at[part(s)], s_out.at[s])

    get_s(0).start()
    get_w(0).start()
    get_w(1).start()
    get_s(1).start()
    get_w(2).start()
    get_w(3).start()
    E = spread(32, 1024)
    E8 = spread(8, 256)
    cls = (lax.broadcasted_iota(jnp.int32, (256, 1024), 1) % 32).astype(F32)
    lb[...] = jnp.zeros_like(lb)

    def hits(t, u):
        rep = dot(samps_t[t].astype(F32).astype(BF), E, ((0,), (0,)))
        hot[t] = jnp.where(rep == cls, 1.0, 0.0).astype(BF)
        return u

    lax.fori_loop(0, STEPS, hits, 0)

    def product(s, n):
        low = jnp.concatenate([stv[b, :, part(s)].reshape(512, 512) for b in range(BLOCKS)], axis=1)
        rhs = jnp.concatenate([wpv[2 * n + i].reshape(2048, 128) for i in range(2)], axis=1)
        return dot(low, rhs)

    def scores(logits, s, n):
        def grouped(v):
            hi = v.astype(BF)
            low = (v - hi.astype(F32)).astype(BF)
            return dot(E8, hi, ((1,), (1,))) + dot(E8, low, ((1,), (1,)))

        cols = pl.ds(pl.multiple_of(n * 256, 256), 256)
        total = jnp.log(grouped(jnp.exp(logits)))
        hit = grouped(logits * hot[:, part(s), cols].reshape(512, 256).astype(F32))
        value = hit - total
        for t in range(STEPS):
            lp[t, pl.ds(pl.multiple_of(n * 8, 8), 8), part(s)] = jnp.where(
                live[:, part(s)] > 0.0, value[:, 128 * t : 128 * t + 128], 0.0
            )

    def trip(j, u):
        @pl.when(j < 2)
        def _():
            get_s(j).wait()

            def lay(b, u):
                for t in range(STEPS):
                    scr[:, t, :] = stv[b, t, part(j)].astype(F32)
                cols = pl.ds(pl.multiple_of(b * 512, 512), 512)
                imgv[part(j), :, cols] = scr[...].astype(BF)
                return u

            lax.fori_loop(0, BLOCKS, lay, 0)
            put(j).start()
            get_w(2 * j).wait()
            get_w(2 * j + 1).wait()

        s, n = j // 2, 2 * (j % 2)
        last = (2 * j + 7) % 8
        la[...] = product(s, n)
        scores(lb[...], last // 4, last % 4)
        lb[...] = product(s, n + 1)
        scores(la[...], s, n)
        return u

    lax.fori_loop(0, 4, trip, 0)
    scores(lb[...], 1, 3)
    put(0).wait()
    put(1).wait()


def on_device(deter, stoch, rows, counts, acts, samps, w_s, w_d, act, w_p):
    vmem = pl.BlockSpec(memory_space=pltpu.VMEM)
    hbm = pl.BlockSpec(memory_space=pl.ANY)
    dma = pltpu.SemaphoreType.DMA
    samps_t = samps.transpose(1, 2, 0)
    states, wp, live = pl.pallas_call(
        gru_kernel,
        name="gru",
        out_shape=(
            jax.ShapeDtypeStruct((4, 4, 256, 512), BF),
            jax.ShapeDtypeStruct((8, 4, 4, 2, 4, 16, 128), BF),
            jax.ShapeDtypeStruct((8, 256), F32),
        ),
        in_specs=[hbm] + [vmem] * 5 + [hbm, hbm, vmem, hbm],
        out_specs=(hbm, hbm, vmem),
        scratch_shapes=[
            pltpu.VMEM((256, 2048), F32),
            pltpu.VMEM((4, 3, 4, 4, 4, 2, 32, 128), BF),
            pltpu.VMEM((4, 3, 4, 4, 4, 2, 16, 128), BF),
            pltpu.VMEM((8, 4, 4, 2, 4, 16, 128), BF),
            pltpu.VMEM((2048, 128), jnp.int32),
            pltpu.VMEM((2048, 128), jnp.int32),
            pltpu.VMEM((128, 1, 128), jnp.int32),
            pltpu.VMEM((128, 1, 128), jnp.int32),
            pltpu.VMEM((256, 128), jnp.int32),
            pltpu.VMEM((4, 256, 512), F32),
            pltpu.VMEM((256, 512), F32),
            pltpu.VMEM((1024, 1024), BF),
            pltpu.VMEM((32, 6144), BF),
            pltpu.VMEM((1024, 32), BF),
            pltpu.VMEM((4, 3, 1024, 512), F32),
            pltpu.VMEM((2, 4, 256, 512), BF),
            dma((7,)), dma((2,)), dma((2,)),
            dma((4, 3)), dma((4, 8, 2)),
            dma((5,)), dma((8, 2)),
            dma((5,)), dma((5,)), dma((6,)),
        ],
        compiler_params=pltpu.CompilerParams(
            collective_id=0, has_side_effects=True, vmem_limit_bytes=63 * 1024 * 1024
        ),
    )(deter, stoch.T, rows.T, counts, acts.T, samps_t, w_s, w_d, act, w_p)
    imagined, logp = pl.pallas_call(
        prior_kernel,
        name="prior",
        out_shape=(
            jax.ShapeDtypeStruct((256, 4, 2048), BF),
            jax.ShapeDtypeStruct((4, 32, 256), F32),
        ),
        in_specs=[hbm, hbm, vmem, vmem],
        out_specs=(hbm, vmem),
        scratch_shapes=[
            pltpu.VMEM((4, 4, 256, 512), BF),
            pltpu.VMEM((8, 4, 4, 2, 4, 16, 128), BF),
            pltpu.VMEM((4, 256, 1024), BF),
            pltpu.VMEM((128, 4, 512), F32),
            pltpu.VMEM((256, 4, 2048), BF),
            pltpu.VMEM((512, 256), F32),
            pltpu.VMEM((512, 256), F32),
            dma((2,)), dma((4,)), dma((2,)),
        ],
        compiler_params=pltpu.CompilerParams(vmem_limit_bytes=60 * 1024 * 1024),
    )(states, wp, live, samps_t)
    return (imagined, logp.transpose(2, 0, 1))


def solution(mesh):
    in_specs = (
        P(("gx", "gy"), None),
        P(("gx", "gy"), None),
        P(("gx", "gy"), None),
        P(("gx", "gy"), None),
        P(("gx", "gy"), None),
        P(("gx", "gy"), None, None),
        P("gy", None),
        P(None, "gy", None),
        P(),
        P("gy", None),
    )
    out_specs = (P(("gx", "gy"), None, None), P(("gx", "gy"), None, None))
    return jax.shard_map(
        on_device, mesh=mesh, in_specs=in_specs, out_specs=out_specs, check_vma=False
    )
```
